256 devices in a mesh: epoch: 16 (over y, x), blend: 16 (over z, core).
Axes of the slice: x: 4, y: 4, z: 8, core: 2. Of those that a mesh axis runs over, the one named last changes fastest.
Arguments:
- visit_flux: bfloat16 [64, 64, 6, 16384], P('epoch', None, None, 'blend'), may hold values from -6 to 6
- visit_precision: bfloat16 [64, 64, 6, 16384], P('epoch', None, None, 'blend'), may hold values from 0.25 to 4
- visit_live: int32 [64, 64], P('epoch'), may hold values 0 or 1
- footprint: int32 [64, 8, 16384], P('blend', None, 'epoch'), may hold values 0 or 1
- source_count: int32 [64], P('blend'), may hold values from 1 to 8
- spectra_init: float32 [64, 8, 6], P('blend'), may hold values from 0.2 to 1.2
- morphology_init: float32 [64, 8, 16384], P('blend', None, 'epoch'), may hold values from 0 to 0.25
Outputs:
- coadd_flux: float32 [64, 6, 16384], P('blend', None, 'epoch')
- spectra: float32 [64, 8, 6], P('blend')
- morphology: float32 [64, 8, 16384], P('blend', None, 'epoch')
The draws below stay inside these ranges and needn't reach their ends.
All inputs are finite; a program needn't handle non-finite values. No bound on the sum of `visit_live` or of `footprint` on one device may be relied on, other than what follows from the above.
Results may differ from the reference program's by a relative error of at most 0.0003.
Values sent between devices are 32-bit elements; how exact they have to be, the bound alone decides.
A program may use at most 64 MiB of HBM per device.

```python
import math
import jax
import jax.numpy as jnp
from jax import lax

PIX = 16384
BANDS = 6
SRC = 8
ITERS = 2
EPOCHS = 64
BLENDS = 64


def with_ends(array, key, smallest, largest):
    dims = array.shape
    place = [jax.random.randint(jax.random.fold_in(key, axis), (), 0, dims[axis]) for axis in range(len(dims))]
    array = array.at[tuple(place)].set(smallest)
    longest = dims.index(max(dims))
    place[longest] = (place[longest] + 1) % dims[longest]
    return array.at[tuple(place)].set(largest)


def shard_levels(rng, shape, pieces, low, top_value):
    def one(position, blocks):
        draws = jax.random.uniform(jax.random.fold_in(jax.random.fold_in(rng, 6), position), (blocks,), jnp.float32, low / len(pieces), top_value / len(pieces))
        return jnp.repeat(jnp.exp(draws), shape[position] // blocks).reshape((-1,) + (1,) * (len(shape) - position - 1))

    gain = one(*pieces[0])
    for cut in pieces[1:]:
        gain = gain * one(*cut)
    return gain


def normal_values(own_key, extent, spread, bound, pieces=(), held_as=jnp.bfloat16):
    loudness = shard_levels(own_key, extent, pieces, -0.22, 0.18) if pieces else 1.0
    result = jax.random.normal(own_key, extent, jnp.float32) * spread * loudness
    return jnp.minimum(jnp.maximum(result, -bound), bound).astype(held_as)


def setup_inputs(seed: int = 0) -> dict:
    key_of = jax.random.split(jax.random.key(seed), 8)
    return {
        "visit_flux": normal_values(key_of[0], (EPOCHS, BLENDS, BANDS, PIX), 1.0, 6.0, ((0, 16), (3, 16))),
        "visit_precision": jnp.clip(jnp.exp(math.log(4.0) - 2.7725887 * jax.random.uniform(key_of[1], (EPOCHS, BLENDS, BANDS, PIX), jnp.float32) ** shard_levels(key_of[1], (EPOCHS, BLENDS, BANDS, PIX), ((0, 16), (3, 16)), -0.2, 0.2)), 0.25, 4.0).astype(jnp.bfloat16),
        "visit_live": with_ends((jax.random.randint(key_of[2], (EPOCHS, BLENDS), 0, 4) < 3).astype(jnp.int32), jax.random.fold_in(key_of[2], 1), 0, 1),
        "footprint": with_ends((jax.random.randint(key_of[3], (BLENDS, SRC, PIX), 0, 2) < 1).astype(jnp.int32), jax.random.fold_in(key_of[3], 1), 0, 1),
        "source_count": with_ends(jax.random.randint(key_of[4], (BLENDS,), 1, SRC + 1), jax.random.fold_in(key_of[4], 1), 1, SRC).astype(jnp.int32),
        "spectra_init": jnp.clip(0.2 + 1 * jax.random.uniform(key_of[5], (BLENDS, SRC, BANDS), jnp.float32) ** shard_levels(key_of[5], (BLENDS, SRC, BANDS), ((0, 16),), -0.2, 0.2), 0.2, 1.2),
        "morphology_init": jnp.clip(0.25 * jax.random.uniform(key_of[6], (BLENDS, SRC, PIX), jnp.float32) ** shard_levels(key_of[6], (BLENDS, SRC, PIX), ((0, 16), (2, 16)), -0.2, 0.2), 0.0, 0.25),
    }


def reference(visit_flux, visit_precision, visit_live, footprint, source_count, spectra_init, morphology_init):
    def accumulate(totals, visit):
        flux_one, precision_one, live_one = visit
        weights = precision_one.astype(jnp.float32) * live_one.astype(jnp.float32)[:, None, None]
        return (totals[0] + weights * flux_one.astype(jnp.float32), totals[1] + weights), None

    zeros = jnp.zeros(visit_flux.shape[1:], jnp.float32)
    (numerator, weight_sum), _ = lax.scan(accumulate, (zeros, zeros), (visit_flux, visit_precision, visit_live))
    coadd_flux = numerator / (1.0 + weight_sum)
    coverage = weight_sum / (1.0 + weight_sum)
    source_live = (jnp.arange(SRC, dtype=jnp.int32)[None, :] < source_count[:, None]).astype(jnp.float32)
    footprint_mask = footprint.astype(jnp.float32) * source_live[:, :, None]
    live_count = source_count.astype(jnp.float32)
    morphology = morphology_init * footprint_mask
    spectra = spectra_init
    highest = lax.Precision.HIGHEST
    for iteration in range(ITERS):
        blend_model = jnp.einsum("bkc,bkp->bcp", spectra, morphology, precision=highest)
        residual = coverage * (coadd_flux - blend_model)
        morph_grad = jnp.einsum("bkc,bcp->bkp", spectra, residual, precision=highest)
        morph_step = 1.0 / (1.0 + live_count[:, None] * jnp.sum(spectra * spectra, axis=2))
        morphology = jnp.maximum(0.0, morphology + morph_grad * morph_step[:, :, None]) * footprint_mask
        blend_model = jnp.einsum("bkc,bkp->bcp", spectra, morphology, precision=highest)
        residual = coverage * (coadd_flux - blend_model)
        spectra_grad = jnp.einsum("bkp,bcp->bkc", morphology, residual, precision=highest)
        morph_norm = jnp.sum(morphology * morphology, axis=2)
        spectra = jnp.maximum(0.0, spectra + spectra_grad / (1.0 + live_count[:, None] * morph_norm)[:, :, None])
    return coadd_flux, spectra, morphology
```

```python
import jax
import jax.numpy as jnp
from jax import lax
from jax.experimental import pallas as pl
from jax.experimental.pallas import tpu as pltpu
from jax.sharding import PartitionSpec as P

ITERS = 2
LANES = 128
F32 = jnp.float32
HIGHEST = lax.Precision.HIGHEST


def kernel(
    flux, prec, live, foot, count, spec, morph,
    coadd_o, spec_o, morph_o,
    fx, pr, live_i, live_b, ft, mo, sp_in, sp_s,
    part, rf, rp, rs, red, rf2, rp2, rs2, zs, zr, fin, co, cv, ar,
    load_sem, small_sem, s1, r1, s2, r2, zsem_s, zsem_r, xsem_s, xsem_r, asem_s, asem_r,
):
    e = lax.axis_index("epoch")
    b = lax.axis_index("blend")
    y, x = lax.div(e, 4), lax.rem(e, 4)
    z, c = lax.div(b, 2), lax.rem(b, 2)

    def mod4(v):
        return lax.rem(v, 4)

    order = [
        mod4(x + 2), 4 + mod4(y + 2),
        mod4(x + 1), mod4(x + 3), 4 + mod4(y + 1), 4 + mod4(y + 3),
        x, 4 + y,
    ]

    small = [
        pltpu.make_async_copy(live, live_i, small_sem.at[0]),
        pltpu.make_async_copy(spec, sp_in, small_sem.at[1]),
        pltpu.make_async_copy(foot, ft, small_sem.at[2]),
        pltpu.make_async_copy(morph, mo, small_sem.at[3]),
    ]
    small[0].start()
    loads = []
    for i, t in enumerate(order):
        lanes = pl.ds(pl.multiple_of(t * LANES, LANES), LANES)
        pair = (
            pltpu.make_async_copy(flux.at[:, :, :, lanes], fx.at[i], load_sem.at[0, i]),
            pltpu.make_async_copy(prec.at[:, :, :, lanes], pr.at[i], load_sem.at[1, i]),
        )
        for cp in pair:
            cp.start()
        loads.append(pair)
    for cp in small[1:]:
        cp.start()

    barrier = pltpu.get_barrier_semaphore()
    for d in range(1, 16):
        pl.semaphore_signal(barrier, inc=1, device_id={"epoch": lax.rem(e + d, 16), "blend": b})
        pl.semaphore_signal(barrier, inc=1, device_id={"epoch": e, "blend": lax.rem(b + d, 16)})

    small[0].wait()
    live_f = live_i[...].astype(F32)
    for v in range(4):
        pick = (lax.broadcasted_iota(jnp.int32, (4, LANES), 0) == v).astype(F32)
        live_b[v] = lax.dot_general(
            live_f, pick, (((0,), (0,)), ((), ())), preferred_element_type=F32
        )

    low = lax.broadcasted_iota(jnp.int32, (8, LANES), 0) < 4

    def local_sums(i):
        for cp in loads[i]:
            cp.wait()
        t = order[i]

        def body(g, _):
            rows = pl.ds(pl.multiple_of(g * 16, 16), 16)
            for cpair in range(3):
                sums = []
                for cc in range(2):
                    band = 2 * cpair + cc
                    num = wsum = None
                    for v in range(4):
                        w = pr[i, v, band, rows, :].astype(F32) * live_b[v, rows, :]
                        n = w * fx[i, v, band, rows, :].astype(F32)
                        num = n if num is None else num + n
                        wsum = w if wsum is None else wsum + w
                    sums.append((num, wsum))
                for q in range(2):
                    for zz in range(2):
                        even = sums[0][q][8 * zz : 8 * zz + 8]
                        odd = sums[1][q][8 * zz : 8 * zz + 8]
                        part[t, q, 0, 2 * g + zz, cpair] = jnp.where(low, even, pltpu.roll(odd, 4, 0))
                        part[t, q, 1, 2 * g + zz, cpair] = jnp.where(low, pltpu.roll(even, 4, 0), odd)
            return 0

        lax.fori_loop(0, 4, body, 0)

    def at_x(d):
        return {"epoch": 4 * y + mod4(x + d), "blend": b}

    def at_y(d):
        return {"epoch": 4 * mod4(y + d) + x, "blend": b}

    def rdma(src, dst, ssem, rsem, dev):
        return pltpu.make_async_remote_copy(
            src, dst, ssem, rsem, device_id=dev, device_id_type=pl.DeviceIdType.MESH
        )

    pos1 = (x, y)
    at1 = (at_x, at_y)

    def chunk1(h, d, q):
        return part.at[4 * h + mod4(pos1[h] + d), q]

    def msg1(h, kind, direction):
        d = 1 if direction == 0 else 3
        if kind == 0:
            src, dst = chunk1(h, 2, direction), rf.at[h, direction]
        elif kind == 1:
            src, dst = chunk1(h, d, 1 - direction), rp.at[h, direction]
        else:
            src, dst = chunk1(h, d, direction), rs.at[h, direction]
        n = 6 * h + 2 * kind + direction
        return rdma(src, dst, s1.at[n], r1.at[n], at1[h](d))

    local_sums(0)
    local_sums(1)
    pl.semaphore_wait(barrier, 30)
    for h in range(2):
        for direction in range(2):
            msg1(h, 0, direction).start()
    for i in (2, 3, 4, 5):
        local_sums(i)
        h, direction = (i - 2) // 2, (i - 2) % 2
        msg1(h, 1, direction).start()
    local_sums(6)
    local_sums(7)

    def add_into(dst, *srcs):
        def body(j, _):
            a, m = lax.div(j, 8), lax.rem(j, 8)
            total = dst[a, m]
            for s in srcs:
                total = total + s[a, m]
            dst[a, m] = total
            return 0

        lax.fori_loop(0, 16, body, 0)

    for h in range(2):
        for direction in range(2):
            msg1(h, 0, direction).wait_recv()
            d = 1 if direction == 0 else 3
            add_into(chunk1(h, d, direction), rf.at[h, direction])
            msg1(h, 2, direction).start()

    for cp in small[1:]:
        cp.wait()
    krow = lax.broadcasted_iota(jnp.int32, (8, 1024), 0)
    for j in range(4):
        rows = pl.ds(8 * j, 8)
        seen = (krow < count[j]).astype(F32) * ft[rows, :].astype(F32)
        ft_f = seen
        mo[rows, :] = mo[rows, :] * ft_f
        cv[pl.ds(32 + 8 * j, 8), :] = ft_f
    sp_s[...] = jnp.zeros_like(sp_s)
    for j in range(4):
        sp_s[0:6, 8 * j : 8 * j + 8] = sp_in[:, j, :]

    pos2 = (y, x)
    at2 = (at_y, at_x)

    def chunk2(h, d, part_of):
        j = mod4(pos2[h] + d)
        return red.at[h, lax.div(j, 2), lax.rem(j, 2), pl.ds(4 * part_of, 4)]

    def msg2(h, kind, direction):
        d = 1 if direction == 0 else 3
        if kind == 0:
            src, dst = chunk2(h, 2, direction), rf2.at[h, direction]
        elif kind == 1:
            src, dst = chunk2(h, d, 1 - direction), rp2.at[h, direction]
        else:
            src, dst = chunk2(h, d, direction), rs2.at[h, direction]
        n = 6 * h + 2 * kind + direction
        return rdma(src, dst, s2.at[n], r2.at[n], at2[h](d))

    for h in range(2):
        for kind in (1, 2):
            for direction in range(2):
                msg1(h, kind, direction).wait_recv()
        mine = 4 * h + pos1[h]

        def total1(j, _, h=h, mine=mine):
            a, m = lax.div(j, 8), lax.rem(j, 8)
            red[h, 0, a, m] = part[mine, 0, a, m] + rs[h, 0, a, m] + rp[h, 1, a, m]
            red[h, 1, a, m] = part[mine, 1, a, m] + rp[h, 0, a, m] + rs[h, 1, a, m]
            return 0

        lax.fori_loop(0, 16, total1, 0)
        for direction in range(2):
            msg2(h, 0, direction).start()
        for direction in range(2):
            msg2(h, 1, direction).start()
    for h in range(2):
        for direction in range(2):
            msg2(h, 0, direction).wait_recv()
            d = 1 if direction == 0 else 3
            dst = chunk2(h, d, direction)
            for m in range(4):
                dst[m] = dst[m] + rf2[h, direction, m]
            msg2(h, 2, direction).start()

    core_to = (lax.rem(y, 2), lax.rem(x, 2))

    def msg_z(h, d):
        zt = lax.rem(z + d, 8)
        return rdma(
            zs.at[h, zt], zr.at[h, b], zsem_s.at[h], zsem_r.at[h],
            {"epoch": e, "blend": 2 * zt + core_to[h]},
        )

    for h in range(2):
        for kind in (1, 2):
            for direction in range(2):
                msg2(h, kind, direction).wait_recv()
        j = pos2[h]
        a, k = lax.div(j, 2), lax.rem(j, 2)
        for m in range(4):
            zs[h, m] = red[h, a, k, m] + rs2[h, 0, m] + rp2[h, 1, m]
            zs[h, 4 + m] = red[h, a, k, 4 + m] + rp2[h, 0, m] + rs2[h, 1, m]
        for d in (4, 3, 5, 2, 6, 1, 7):
            msg_z(h, d).start()

        @pl.when(core_to[h] == c)
        def _(h=h):
            zr[h, b] = zs[h, z]

        @pl.when(core_to[h] != c)
        def _(h=h):
            msg_z(h, 0).start()

    quantity = (lax.div(y, 2), lax.div(x, 2))
    tile = (x, 4 + y)

    def msg_x(h, d):
        et = lax.rem(e + d, 16)
        return rdma(
            zr.at[h, et], fin.at[8 * quantity[h] + tile[h]], xsem_s.at[h], xsem_r.at[h],
            {"epoch": et, "blend": b},
        )

    def wait_bytes(ref, sem):
        pltpu.make_async_copy(ref, ref, sem).wait()

    for h in range(2):

        @pl.when(core_to[h] == c)
        def _(h=h):
            wait_bytes(zr.at[h, pl.ds(0, 15)], zsem_r.at[h])
            for d in range(1, 16):
                msg_x(h, d).start()
            fin[8 * quantity[h] + tile[h]] = zr[h, e]

    for h in range(2):

        @pl.when(core_to[h] == c)
        def _(h=h):
            wait_bytes(fin.at[pl.ds(0, 7)], xsem_r.at[h])

        @pl.when(core_to[h] != c)
        def _(h=h):
            wait_bytes(fin.at[pl.ds(0, 8)], xsem_r.at[h])

    for t in range(8):
        for cpair in range(3):
            rows, lanes = slice(8 * cpair, 8 * cpair + 8), slice(128 * t, 128 * t + 128)
            wsum = fin[8 + t, cpair]
            inv = 1.0 / (1.0 + wsum)
            co[rows, lanes] = fin[t, cpair] * inv
            cv[rows, lanes] = wsum * inv
    coadd_o[...] = co[...]

    lane = lax.broadcasted_iota(jnp.int32, (8, 32), 1)
    row = lax.broadcasted_iota(jnp.int32, (8, 32), 0)
    own = (lax.div(lane, 8) == lax.rem(row, 4)).astype(F32)
    own3 = jnp.concatenate([own] * 3, axis=0)
    lane1 = lax.div(lax.broadcasted_iota(jnp.int32, (1, 32), 1), 8)
    live_row = jnp.zeros((1, 32), F32)
    for j in range(4):
        live_row = jnp.where(lane1 == j, count[j].astype(F32), live_row)
    gather = (
        lax.broadcasted_iota(jnp.int32, (8, 24), 0)
        == lax.div(lax.broadcasted_iota(jnp.int32, (8, 24), 1), 4)
    ).astype(F32)
    is_norm = row == 6
    bands = row < 6

    def dot(a, bb, ca, cb):
        return lax.dot_general(
            a, bb, (((ca,), (cb,)), ((), ())), precision=HIGHEST, preferred_element_type=F32
        )

    coadd = co[...]
    cover = cv[0:24, :]
    mask = cv[32:64, :]
    morphology = mo[...]
    spectra = sp_s[:, 0:32]
    for it in range(ITERS):
        wide = jnp.concatenate(
            [
                jnp.where(
                    row < 4,
                    jnp.broadcast_to(spectra[2 * p : 2 * p + 1], (8, 32)),
                    jnp.broadcast_to(spectra[2 * p + 1 : 2 * p + 2], (8, 32)),
                )
                for p in range(3)
            ],
            axis=0,
        ) * own3
        step = 1.0 / (1.0 + live_row * jnp.sum(spectra * spectra, axis=0, keepdims=True))
        residual = cover * (coadd - dot(wide, morphology, 1, 0))
        morphology = jnp.maximum(0.0, morphology + dot(wide * step, residual, 0, 0)) * mask
        residual = cover * (coadd - dot(wide, morphology, 1, 0))
        grad = dot(gather, dot(residual, morphology, 1, 1) * own3, 1, 0)
        norm = dot(jnp.ones((8, 1024), F32), morphology * morphology, 1, 1)
        ar[it, e] = jnp.zeros((8, LANES), F32)
        ar[it, e, :, 0:32] = jnp.where(is_norm, norm, grad)
        for d in range(1, 16):
            rdma(
                ar.at[it, e], ar.at[it, e], asem_s.at[it], asem_r.at[it],
                {"epoch": lax.rem(e + d, 16), "blend": b},
            ).start()
        if it == ITERS - 1:
            morph_o[...] = morphology
        wait_bytes(ar.at[it, pl.ds(0, 15)], asem_r.at[it])
        total = ar[it, 0, :, 0:32]
        for d in range(1, 16):
            total = total + ar[it, d, :, 0:32]
        spectra = jnp.where(
            bands,
            jnp.maximum(0.0, spectra + total / (1.0 + live_row * total[6:7])),
            0.0,
        )
    for j in range(4):
        spec_o[:, j, :] = spectra[0:6, 8 * j : 8 * j + 8]

    for h in range(2):
        for kind in range(3):
            for direction in range(2):
                msg1(h, kind, direction).wait_send()
                msg2(h, kind, direction).wait_send()

        @pl.when(core_to[h] == c)
        def _(h=h):
            wait_bytes(zs.at[h, pl.ds(0, 7)], zsem_s.at[h])
            wait_bytes(zr.at[h, pl.ds(0, 15)], xsem_s.at[h])

        @pl.when(core_to[h] != c)
        def _(h=h):
            wait_bytes(zs.at[h, pl.ds(0, 8)], zsem_s.at[h])

    for it in range(ITERS):
        wait_bytes(ar.at[it, pl.ds(0, 15)], asem_s.at[it])


def on_device(
    visit_flux, visit_precision, visit_live, footprint, source_count, spectra_init, morphology_init
):
    tile = (8, LANES)
    hbm = pl.BlockSpec(memory_space=pl.ANY)
    vmem = pl.BlockSpec(memory_space=pltpu.VMEM)
    dma = pltpu.SemaphoreType.DMA
    coadd, spectra, morphology = pl.pallas_call(
        kernel,
        name="coadd_deblend",
        out_shape=(
            jax.ShapeDtypeStruct((24, 1024), F32),
            jax.ShapeDtypeStruct((6, 4, 8), F32),
            jax.ShapeDtypeStruct((32, 1024), F32),
        ),
        in_specs=[hbm, hbm, hbm, hbm, pl.BlockSpec(memory_space=pltpu.SMEM), hbm, hbm],
        out_specs=(vmem, vmem, vmem),
        scratch_shapes=[
            pltpu.VMEM((8, 4, 6, 64, LANES), jnp.bfloat16),
            pltpu.VMEM((8, 4, 6, 64, LANES), jnp.bfloat16),
            pltpu.VMEM((4, 64), jnp.int32),
            pltpu.VMEM((4, 64, LANES), F32),
            pltpu.VMEM((32, 1024), jnp.int32),
            pltpu.VMEM((32, 1024), F32),
            pltpu.VMEM((6, 4, 8), F32),
            pltpu.VMEM(tile, F32),
            pltpu.VMEM((8, 2, 2, 8, 3, *tile), F32),
            pltpu.VMEM((2, 2, 2, 8, 3, *tile), F32),
            pltpu.VMEM((2, 2, 2, 8, 3, *tile), F32),
            pltpu.VMEM((2, 2, 2, 8, 3, *tile), F32),
            pltpu.VMEM((2, 2, 2, 8, 3, *tile), F32),
            pltpu.VMEM((2, 2, 4, 3, *tile), F32),
            pltpu.VMEM((2, 2, 4, 3, *tile), F32),
            pltpu.VMEM((2, 2, 4, 3, *tile), F32),
            pltpu.VMEM((2, 8, 3, *tile), F32),
            pltpu.VMEM((2, 16, 3, *tile), F32),
            pltpu.VMEM((16, 3, *tile), F32),
            pltpu.VMEM((24, 1024), F32),
            pltpu.VMEM((64, 1024), F32),
            pltpu.VMEM((ITERS, 16, *tile), F32),
            dma((2, 8)), dma((4,)),
            dma((12,)), dma((12,)), dma((12,)), dma((12,)),
            dma((2,)), dma((2,)), dma((2,)), dma((2,)),
            dma((ITERS,)), dma((ITERS,)),
        ],
        compiler_params=pltpu.CompilerParams(
            collective_id=0, has_side_effects=True, vmem_limit_bytes=40 * 1024 * 1024
        ),
    )(
        jnp.transpose(visit_flux, (0, 2, 1, 3)),
        jnp.transpose(visit_precision, (0, 2, 1, 3)),
        visit_live,
        footprint.reshape(32, 1024),
        source_count,
        jnp.transpose(spectra_init, (2, 0, 1)),
        morphology_init.reshape(32, 1024),
    )
    return (
        jnp.transpose(coadd.reshape(6, 4, 1024), (1, 0, 2)),
        jnp.transpose(spectra, (1, 2, 0)),
        morphology.reshape(4, 8, 1024),
    )


def solution(mesh):
    in_specs = (
        P("epoch", None, None, "blend"),
        P("epoch", None, None, "blend"),
        P("epoch", None),
        P("blend", None, "epoch"),
        P("blend"),
        P("blend", None, None),
        P("blend", None, "epoch"),
    )
    out_specs = (P("blend", None, "epoch"), P("blend", None, None), P("blend", None, "epoch"))
    return jax.shard_map(
        on_device, mesh=mesh, in_specs=in_specs, out_specs=out_specs, check_vma=False
    )
```

```python
import jax
import jax.numpy as jnp
from jax import lax
from jax.experimental import pallas as pl
from jax.experimental.pallas import tpu as pltpu
from jax.sharding import PartitionSpec as P

ITERS = 2
LANES = 128
F32 = jnp.float32
HIGHEST = lax.Precision.HIGHEST
HOPS = (0, 1, 2, 1)
FAR_FIRST = sorted(
    [(dy, dx) for dy in range(4) for dx in range(4) if dy or dx],
    key=lambda d: -HOPS[d[0]] - HOPS[d[1]],
)


def kernel(
    flux, prec, live, foot, count_in, spec, morph,
    coadd_o, spec_o, morph_o,
    fx, pr, live_i, live_b, ft, mo, sp_in, sp_s,
    part, rf, rp, rs, red, rf2, rp2, rs2, zs, fin, co, cv, ar, mout, sout,
    count, load_sem, small_sem, ready, out_sem, s1, r1, s1s, r1s, s2, r2, zsem_s, zsem_r, asem_s, asem_r,
):
    e = lax.axis_index("epoch")
    b = lax.axis_index("blend")
    y, x = lax.div(e, 4), lax.rem(e, 4)
    z, c = lax.div(b, 2), lax.rem(b, 2)

    def mod4(v):
        return lax.rem(v, 4)

    order = [
        mod4(x + 2), 4 + mod4(y + 2),
        mod4(x + 1), mod4(x + 3), 4 + mod4(y + 1), 4 + mod4(y + 3),
        x, 4 + y,
    ]
    small = [
        pltpu.make_async_copy(live, live_i, small_sem.at[0]),
        pltpu.make_async_copy(spec, sp_in, small_sem.at[1]),
        pltpu.make_async_copy(foot, ft, small_sem.at[2]),
        pltpu.make_async_copy(morph, mo, small_sem.at[3]),
        pltpu.make_async_copy(count_in, count, small_sem.at[4]),
    ]
    small[0].start()
    loads = []
    for i, t in enumerate(order):
        lanes = pl.ds(pl.multiple_of(t * LANES, LANES), LANES)
        pair = (
            pltpu.make_async_copy(flux.at[:, :, :, lanes], fx.at[i], load_sem.at[0, i]),
            pltpu.make_async_copy(prec.at[:, :, :, lanes], pr.at[i], load_sem.at[1, i]),
        )
        if i < 2:
            for cp in pair:
                cp.start()
        loads.append(pair)

    barrier = pltpu.get_barrier_semaphore()
    for d in range(1, 16):
        pl.semaphore_signal(barrier, inc=1, device_id={"epoch": lax.rem(e + d, 16), "blend": b})
        pl.semaphore_signal(barrier, inc=1, device_id={"epoch": e, "blend": lax.rem(b + d, 16)})
    for pair in loads[2:]:
        for cp in pair:
            cp.start()
    for cp in small[1:]:
        cp.start()
    small[0].wait()
    live_f = live_i[...].astype(F32)
    pick = (
        lax.broadcasted_iota(jnp.int32, (4, 4 * LANES), 0)
        == lax.div(lax.broadcasted_iota(jnp.int32, (4, 4 * LANES), 1), LANES)
    ).astype(F32)
    spread = lax.dot_general(
        live_f, pick, (((0,), (0,)), ((), ())), preferred_element_type=F32
    )
    for v in range(4):
        live_b[v] = spread[:, LANES * v : LANES * v + LANES]

    low = lax.broadcasted_iota(jnp.int32, (8, LANES), 0) < 4

    def local_sums(i):
        for cp in loads[i]:
            cp.wait()
        t = order[i]

        def body(g, _):
            rows = pl.ds(pl.multiple_of(g * 16, 16), 16)
            for cpair in range(3):
                sums = []
                for cc in range(2):
                    band = 2 * cpair + cc
                    num = wsum = None
                    for v in range(4):
                        w = pr[i, v, band, rows, :].astype(F32) * live_b[v, rows, :]
                        n = w * fx[i, v, band, rows, :].astype(F32)
                        num = n if num is None else num + n
                        wsum = w if wsum is None else wsum + w
                    sums.append((num, wsum))
                for q in range(2):
                    for zz in range(2):
                        even = sums[0][q][8 * zz : 8 * zz + 8]
                        odd = sums[1][q][8 * zz : 8 * zz + 8]
                        part[t, q, 0, 2 * g + zz, cpair] = jnp.where(low, even, pltpu.roll(odd, 4, 0))
                        part[t, q, 1, 2 * g + zz, cpair] = jnp.where(low, pltpu.roll(even, 4, 0), odd)
            return 0

        lax.fori_loop(0, 4, body, 0)

    def at_x(d):
        return {"epoch": 4 * y + mod4(x + d), "blend": b}

    def at_y(d):
        return {"epoch": 4 * mod4(y + d) + x, "blend": b}

    def rdma(src, dst, ssem, rsem, dev):
        return pltpu.make_async_remote_copy(
            src, dst, ssem, rsem, device_id=dev, device_id_type=pl.DeviceIdType.MESH
        )

    pos1 = (x, y)
    at1 = (at_x, at_y)

    def chunk1(h, d, q):
        return part.at[4 * h + mod4(pos1[h] + d), q]

    def msg1(h, kind, direction):
        d = 1 if direction == 0 else 3
        if kind == 0:
            src, dst = chunk1(h, 2, direction), rf.at[h, direction]
        else:
            src, dst = chunk1(h, d, 1 - direction), rp.at[h, direction]
        n = 4 * h + 2 * kind + direction
        return rdma(src, dst, s1.at[n], r1.at[n], at1[h](d))

    pos2 = (y, x)
    own_q = tuple(lax.div(p, 2) for p in pos2)
    own_c = tuple(lax.rem(p, 2) for p in pos2)

    def sum1(h, q, piece):
        first = jnp.where(own_q[h] == q, 1 - own_c[h], own_c[h])
        cc = first if piece == 0 else 1 - first
        dev = {"epoch": jnp.where(
            h == 0, 4 * y + mod4(x + 1 + 2 * q), 4 * mod4(y + 1 + 2 * q) + x), "blend": b}
        return rdma(
            part.at[4 * h + mod4(pos1[h] + 1 + 2 * q), q, cc], rs.at[h, q, cc],
            s1s.at[h, q, piece], r1s.at[h, q, piece], dev,
        )
    local_sums(0)
    local_sums(1)
    pl.semaphore_wait(barrier, 30)
    for d in range(1, 16):
        pl.semaphore_signal(ready, inc=1, device_id={"epoch": e, "blend": lax.rem(b + d, 16)})
    for h in range(2):
        for direction in range(2):
            msg1(h, 0, direction).start()
    for i in (2, 3, 4, 5):
        local_sums(i)
        h, direction = (i - 2) // 2, (i - 2) % 2
        msg1(h, 1, direction).start()
    local_sums(6)
    local_sums(7)

    def add_into(dst, *srcs):
        def body(j, _):
            a, m = lax.div(j, 8), lax.rem(j, 8)
            total = dst[a, m]
            for s in srcs:
                total = total + s[a, m]
            dst[a, m] = total
            return 0

        lax.fori_loop(0, 16, body, 0)
    for h in range(2):
        for direction in range(2):
            msg1(h, 0, direction).wait_recv()
            d = 1 if direction == 0 else 3
            add_into(chunk1(h, d, direction), rf.at[h, direction])
            for piece in range(2):
                sum1(h, direction, piece).start()
    for cp in small[1:]:
        cp.wait()
    krow = lax.broadcasted_iota(jnp.int32, (8, 1024), 0)
    for j in range(4):
        rows = pl.ds(8 * j, 8)
        seen = (krow < count[j]).astype(F32) * ft[rows, :].astype(F32)
        ft_f = seen
        mo[rows, :] = mo[rows, :] * ft_f
        cv[pl.ds(32 + 8 * j, 8), :] = ft_f
    sp_s[...] = jnp.zeros_like(sp_s)
    for j in range(4):
        sp_s[0:6, 8 * j : 8 * j + 8] = sp_in[:, j, :]

    at2 = (at_y, at_x)

    def chunk2(h, d, part_of):
        j = mod4(pos2[h] + d)
        return red.at[h, lax.div(j, 2), lax.rem(j, 2), pl.ds(4 * part_of, 4)]

    def msg2(h, kind, direction):
        d = 1 if direction == 0 else 3
        if kind == 0:
            src, dst = chunk2(h, 2, direction), rf2.at[h, direction]
        elif kind == 1:
            src, dst = chunk2(h, d, 1 - direction), rp2.at[h, direction]
        else:
            src, dst = chunk2(h, d, direction), rs2.at[h, direction]
        n = 6 * h + 2 * kind + direction
        return rdma(src, dst, s2.at[n], r2.at[n], at2[h](d))
    def total1(h, q, cc):
        mine = 4 * h + pos1[h]

        def body(m, _):
            red[h, q, cc, m] = part[mine, q, cc, m] + rs[h, q, cc, m] + rp[h, 1 - q, cc, m]
            return 0

        lax.fori_loop(0, 8, body, 0)

    for h in range(2):
        for direction in range(2):
            msg1(h, 1, direction).wait_recv()
    for h in range(2):
        sum1(h, 1 - own_q[h], 0).wait_recv()
        total1(h, 1 - own_q[h], own_c[h])
        for direction in range(2):
            msg2(h, 0, direction).start()
    for h in range(2):
        sum1(h, own_q[h], 0).wait_recv()
        total1(h, own_q[h], 1 - own_c[h])
        sum1(h, 1 - own_q[h], 1).wait_recv()
        total1(h, 1 - own_q[h], 1 - own_c[h])
        for direction in range(2):
            msg2(h, 1, direction).start()
    for h in range(2):
        for direction in range(2):
            msg2(h, 0, direction).wait_recv()
            d = 1 if direction == 0 else 3
            dst = chunk2(h, d, direction)
            for m in range(4):
                dst[m] = dst[m] + rf2[h, direction, m]
            msg2(h, 2, direction).start()

    core_to = (lax.rem(y, 2), lax.rem(x, 2))

    quantity = (lax.div(y, 2), lax.div(x, 2))
    tile = (x, 4 + y)

    def wait_bytes(ref, sem):
        pltpu.make_async_copy(ref, ref, sem).wait()

    def msg_z(h, d):
        zt = lax.rem(z + d, 8)
        return rdma(
            zs.at[h, zt], fin.at[8 * quantity[h] + tile[h]], zsem_s.at[h], zsem_r.at[h],
            {"epoch": b, "blend": 2 * zt + core_to[h]},
        )
    for h in range(2):
        for kind in (1, 2):
            for direction in range(2):
                msg2(h, kind, direction).wait_recv()
        sum1(h, own_q[h], 1).wait_recv()
        total1(h, own_q[h], own_c[h])
        if h == 0:
            pl.semaphore_wait(ready, 15)
        j = pos2[h]
        a, k = lax.div(j, 2), lax.rem(j, 2)
        for m in range(4):
            zs[h, m] = red[h, a, k, m] + rs2[h, 0, m] + rp2[h, 1, m]
            zs[h, 4 + m] = red[h, a, k, 4 + m] + rp2[h, 0, m] + rs2[h, 1, m]
        for d in (4, 3, 5, 2, 6, 1, 7):
            msg_z(h, d).start()

        here = (core_to[h] == c) & (e == b)

        @pl.when(here)
        def _(h=h):
            fin[8 * quantity[h] + tile[h]] = zs[h, z]

        @pl.when(jnp.logical_not(here))
        def _(h=h):
            msg_z(h, 0).start()
    for h in range(2):
        here = (core_to[h] == c) & (e == b)
        @pl.when(here)
        def _(h=h):
            wait_bytes(fin.at[pl.ds(0, 7)], zsem_r.at[h])

        @pl.when(jnp.logical_not(here))
        def _(h=h):
            wait_bytes(fin.at[pl.ds(0, 8)], zsem_r.at[h])
    for t in range(8):
        for cpair in range(3):
            rows, lanes = slice(8 * cpair, 8 * cpair + 8), slice(128 * t, 128 * t + 128)
            wsum = fin[8 + t, cpair]
            inv = 1.0 / (1.0 + wsum)
            co[rows, lanes] = fin[t, cpair] * inv
            cv[rows, lanes] = wsum * inv
    coadd_out = pltpu.make_async_copy(co, coadd_o, out_sem.at[0])
    coadd_out.start()

    lane = lax.broadcasted_iota(jnp.int32, (8, 32), 1)
    row = lax.broadcasted_iota(jnp.int32, (8, 32), 0)
    own = (lax.div(lane, 8) == lax.rem(row, 4)).astype(F32)
    own3 = jnp.concatenate([own] * 3, axis=0)
    lane1 = lax.div(lax.broadcasted_iota(jnp.int32, (1, 32), 1), 8)
    live_row = jnp.zeros((1, 32), F32)
    for j in range(4):
        live_row = jnp.where(lane1 == j, count[j].astype(F32), live_row)
    gather = (
        lax.broadcasted_iota(jnp.int32, (8, 24), 0)
        == lax.div(lax.broadcasted_iota(jnp.int32, (8, 24), 1), 4)
    ).astype(F32)
    is_norm = row == 6
    bands = row < 6

    def dot(a, bb, ca, cb):
        return lax.dot_general(
            a, bb, (((ca,), (cb,)), ((), ())), precision=HIGHEST, preferred_element_type=F32
        )
    coadd = co[...]
    cover = cv[0:24, :]
    mask = cv[32:64, :]
    morphology = mo[...]
    spectra = sp_s[:, 0:32]
    for it in range(ITERS):
        wide = jnp.concatenate(
            [
                jnp.where(
                    row < 4,
                    jnp.broadcast_to(spectra[2 * p : 2 * p + 1], (8, 32)),
                    jnp.broadcast_to(spectra[2 * p + 1 : 2 * p + 2], (8, 32)),
                )
                for p in range(3)
            ],
            axis=0,
        ) * own3
        step = 1.0 / (1.0 + live_row * jnp.sum(spectra * spectra, axis=0, keepdims=True))
        residual = cover * (coadd - dot(wide, morphology, 1, 0))
        morphology = jnp.maximum(0.0, morphology + dot(wide * step, residual, 0, 0)) * mask
        residual = cover * (coadd - dot(wide, morphology, 1, 0))
        grad = dot(gather, dot(residual, morphology, 1, 1) * own3, 1, 0)
        norm = dot(jnp.ones((8, 1024), F32), morphology * morphology, 1, 1)
        ar[it, e] = jnp.zeros((8, LANES), F32)
        ar[it, e, :, 0:32] = jnp.where(is_norm, norm, grad)
        for dy, dx in FAR_FIRST:
            rdma(
                ar.at[it, e], ar.at[it, e], asem_s.at[it], asem_r.at[it],
                {"epoch": 4 * mod4(y + dy) + mod4(x + dx), "blend": b},
            ).start()
        if it == ITERS - 1:
            mout[...] = morphology
            morph_out = pltpu.make_async_copy(mout, morph_o, out_sem.at[1])
            morph_out.start()
        wait_bytes(ar.at[it, pl.ds(0, 15)], asem_r.at[it])
        total = ar[it, 0, :, 0:32]
        for d in range(1, 16):
            total = total + ar[it, d, :, 0:32]
        spectra = jnp.where(
            bands,
            jnp.maximum(0.0, spectra + total / (1.0 + live_row * total[6:7])),
            0.0,
        )
    for j in range(4):
        sout[:, j, :] = spectra[0:6, 8 * j : 8 * j + 8]
    spec_out = pltpu.make_async_copy(sout, spec_o, out_sem.at[2])
    spec_out.start()
    for h in range(2):
        for direction in range(2):
            for kind in range(2):
                msg1(h, kind, direction).wait_send()
                sum1(h, direction, kind).wait_send()
            for kind in range(3):
                msg2(h, kind, direction).wait_send()

        here = (core_to[h] == c) & (e == b)
        @pl.when(here)
        def _(h=h):
            wait_bytes(zs.at[h, pl.ds(0, 7)], zsem_s.at[h])

        @pl.when(jnp.logical_not(here))
        def _(h=h):
            wait_bytes(zs.at[h, pl.ds(0, 8)], zsem_s.at[h])

    for it in range(ITERS):
        wait_bytes(ar.at[it, pl.ds(0, 15)], asem_s.at[it])
    for cp in (coadd_out, morph_out, spec_out):
        cp.wait()


def on_device(
    visit_flux, visit_precision, visit_live, footprint, source_count, spectra_init, morphology_init
):
    tile = (8, LANES)
    hbm = pl.BlockSpec(memory_space=pl.ANY)
    dma = pltpu.SemaphoreType.DMA
    coadd, spectra, morphology = pl.pallas_call(
        kernel,
        name="coadd_deblend",
        out_shape=(
            jax.ShapeDtypeStruct((24, 1024), F32),
            jax.ShapeDtypeStruct((6, 4, 8), F32),
            jax.ShapeDtypeStruct((32, 1024), F32),
        ),
        in_specs=[hbm] * 7,
        out_specs=(hbm, hbm, hbm),
        scratch_shapes=[
            pltpu.VMEM((8, 4, 6, 64, LANES), jnp.bfloat16),
            pltpu.VMEM((8, 4, 6, 64, LANES), jnp.bfloat16),
            pltpu.VMEM((4, 64), jnp.int32),
            pltpu.VMEM((4, 64, LANES), F32),
            pltpu.VMEM((32, 1024), jnp.int32),
            pltpu.VMEM((32, 1024), F32),
            pltpu.VMEM((6, 4, 8), F32),
            pltpu.VMEM(tile, F32),
            pltpu.VMEM((8, 2, 2, 8, 3, *tile), F32),
            pltpu.VMEM((2, 2, 2, 8, 3, *tile), F32),
            pltpu.VMEM((2, 2, 2, 8, 3, *tile), F32),
            pltpu.VMEM((2, 2, 2, 8, 3, *tile), F32),
            pltpu.VMEM((2, 2, 2, 8, 3, *tile), F32),
            pltpu.VMEM((2, 2, 4, 3, *tile), F32),
            pltpu.VMEM((2, 2, 4, 3, *tile), F32),
            pltpu.VMEM((2, 2, 4, 3, *tile), F32),
            pltpu.VMEM((2, 8, 3, *tile), F32),
            pltpu.VMEM((16, 3, *tile), F32),
            pltpu.VMEM((24, 1024), F32),
            pltpu.VMEM((64, 1024), F32),
            pltpu.VMEM((ITERS, 16, *tile), F32),
            pltpu.VMEM((32, 1024), F32),
            pltpu.VMEM((6, 4, 8), F32),
            pltpu.SMEM((4,), jnp.int32),
            dma((2, 8)), dma((5,)), pltpu.SemaphoreType.REGULAR, dma((3,)),
            dma((8,)), dma((8,)), dma((2, 2, 2)), dma((2, 2, 2)), dma((12,)), dma((12,)),
            dma((2,)), dma((2,)),
            dma((ITERS,)), dma((ITERS,)),
        ],
        compiler_params=pltpu.CompilerParams(
            collective_id=0, has_side_effects=True, vmem_limit_bytes=67043328
        ),
    )(
        jnp.transpose(visit_flux, (0, 2, 1, 3)),
        jnp.transpose(visit_precision, (0, 2, 1, 3)),
        visit_live,
        footprint.reshape(32, 1024),
        source_count,
        jnp.transpose(spectra_init, (2, 0, 1)),
        morphology_init.reshape(32, 1024),
    )
    return (
        jnp.transpose(coadd.reshape(6, 4, 1024), (1, 0, 2)),
        jnp.transpose(spectra, (1, 2, 0)),
        morphology.reshape(4, 8, 1024),
    )


def solution(mesh):
    in_specs = (
        P("epoch", None, None, "blend"),
        P("epoch", None, None, "blend"),
        P("epoch", None),
        P("blend", None, "epoch"),
        P("blend"),
        P("blend", None, None),
        P("blend", None, "epoch"),
    )
    out_specs = (P("blend", None, "epoch"), P("blend", None, None), P("blend", None, "epoch"))
    return jax.shard_map(
        on_device, mesh=mesh, in_specs=in_specs, out_specs=out_specs, check_vma=False
    )
```

```python
import jax
import jax.numpy as jnp
from jax import lax
from jax.experimental import pallas as pl
from jax.experimental.pallas import tpu as pltpu
from jax.sharding import PartitionSpec as P

ITERS = 2
LANES = 128
F32 = jnp.float32
HOPS = (0, 1, 2, 1)
FAR_FIRST = sorted(
    [(dy, dx) for dy in range(4) for dx in range(4) if dy or dx],
    key=lambda d: -HOPS[d[0]] - HOPS[d[1]],
)


def kernel(
    flux, prec, live, foot, count_in, spec, morph,
    coadd_o, spec_o, morph_o,
    fp, live_i, live_b, ft, mo, sp_in, sp_s,
    part, rf, rp, rs, red, rf2, rp2, rs2, zs, fin, co, cv, mask, mph, rsd, ar,
    count, load_sem, small_sem, waves, sent, r1, rp_sem, r1s, r2, zsem_s, zsem_r, asem_r,
):
    e = lax.axis_index("epoch")
    b = lax.axis_index("blend")
    y, x = lax.div(e, 4), lax.rem(e, 4)
    z, c = lax.div(b, 2), lax.rem(b, 2)

    def mod4(v):
        return lax.rem(v, 4)

    def wait_bytes(ref, sem):
        pltpu.make_async_copy(ref, ref, sem).wait()

    order = [
        mod4(x + 2), 4 + mod4(y + 2),
        mod4(x + 1), mod4(x + 3), 4 + mod4(y + 1), 4 + mod4(y + 3),
        x, 4 + y,
    ]
    small = [
        pltpu.make_async_copy(live, live_i, small_sem.at[0]),
        pltpu.make_async_copy(spec, sp_in, small_sem.at[1]),
        pltpu.make_async_copy(count_in, count, small_sem.at[4]),
    ]
    for t in range(8):
        lanes = pl.ds(LANES * t, LANES)
        small.append(pltpu.make_async_copy(foot.at[:, lanes], ft.at[t], small_sem.at[2]))
        small.append(pltpu.make_async_copy(morph.at[:, lanes], mo.at[t], small_sem.at[3]))
    small[0].start()
    loads = []
    for i, t in enumerate(order):
        lanes = pl.ds(pl.multiple_of(t * LANES, LANES), LANES)
        group = min(i, 2) if i < 6 else 3
        pair = (
            pltpu.make_async_copy(flux.at[:, :, :, lanes], fp.at[i, 0], load_sem.at[group]),
            pltpu.make_async_copy(prec.at[:, :, :, lanes], fp.at[i, 1], load_sem.at[group]),
        )
        if i < 2:
            for cp in pair:
                cp.start()
        loads.append(pair)

    barrier = pltpu.get_barrier_semaphore()

    def at_x(d):
        return {"epoch": 4 * y + mod4(x + d), "blend": b}

    def at_y(d):
        return {"epoch": 4 * mod4(y + d) + x, "blend": b}

    def at_z(d):
        return {"epoch": e, "blend": lax.rem(b + 2 * d, 16)}

    other_core = {"epoch": e, "blend": 2 * z + 1 - c}
    for dev in (at_x(1), at_x(3), at_y(1), at_y(3), at_z(7), other_core):
        pl.semaphore_signal(barrier, inc=1, device_id=dev)

    def wave(i):
        to = (
            (at_x(1), at_x(3)), (at_y(1), at_y(3)), (at_y(1), at_y(3)),
            (at_z(1),), (at_z(1), at_z(7)), (at_z(2), at_z(6)), (at_z(1), at_z(7)),
            (other_core,),
        )[i]
        for dev in to:
            pl.semaphore_signal(waves.at[i], inc=1, device_id=dev)
        return lambda: pl.semaphore_wait(waves.at[i], len(to))

    for pair in loads[2:]:
        for cp in pair:
            cp.start()
    for cp in small[1:]:
        cp.start()
    small[0].wait()
    live_f = live_i[...].astype(F32)
    pick = (
        lax.broadcasted_iota(jnp.int32, (4, 4 * LANES), 0)
        == lax.div(lax.broadcasted_iota(jnp.int32, (4, 4 * LANES), 1), LANES)
    ).astype(F32)
    spread = lax.dot_general(
        live_f, pick, (((0,), (0,)), ((), ())), preferred_element_type=F32
    )
    for v in range(4):
        live_b[v] = spread[:, LANES * v : LANES * v + LANES]

    low = lax.broadcasted_iota(jnp.int32, (8, LANES), 0) < 4

    def local_sums(i):
        if i in (0, 1, 2, 6):
            wait_bytes(fp.at[pl.ds(i, {2: 4, 6: 2}.get(i, 1))], load_sem.at[min(i, 3)])
        t = order[i]

        def body(g, _):
            rows = pl.ds(pl.multiple_of(g * 16, 16), 16)
            for cpair in range(3):
                sums = []
                for cc in range(2):
                    band = 2 * cpair + cc
                    num = wsum = None
                    for v in range(4):
                        w = fp[i, 1, v, band, rows, :].astype(F32) * live_b[v, rows, :]
                        n = w * fp[i, 0, v, band, rows, :].astype(F32)
                        num = n if num is None else num + n
                        wsum = w if wsum is None else wsum + w
                    sums.append((num, wsum))
                for q in range(2):
                    for zz in range(2):
                        even = sums[0][q][8 * zz : 8 * zz + 8]
                        odd = sums[1][q][8 * zz : 8 * zz + 8]
                        part[t, q, 0, 2 * g + zz, cpair] = jnp.where(low, even, pltpu.roll(odd, 4, 0))
                        part[t, q, 1, 2 * g + zz, cpair] = jnp.where(low, pltpu.roll(even, 4, 0), odd)
            return 0

        lax.fori_loop(0, 4, body, 0)

    def rdma(src, dst, ssem, rsem, dev):
        return pltpu.make_async_remote_copy(
            src, dst, ssem, rsem, device_id=dev, device_id_type=pl.DeviceIdType.MESH
        )

    pos1 = (x, y)
    at1 = (at_x, at_y)

    def chunk1(h, d, q):
        return part.at[4 * h + mod4(pos1[h] + d), q]

    def msg1(h, kind, direction):
        d = 1 if direction == 0 else 3
        if kind == 0:
            src, dst = chunk1(h, 2, direction), rf.at[h, direction]
        else:
            src, dst = chunk1(h, d, 1 - direction), rp.at[h, direction]
        arrived = rp_sem.at[0] if kind == 1 else r1.at[h, direction]
        return rdma(src, dst, sent.at[0], arrived, at1[h](d))

    pos2 = (y, x)
    own_q = tuple(lax.div(p, 2) for p in pos2)
    own_c = tuple(lax.rem(p, 2) for p in pos2)

    def sum1(h, q, piece):
        first = jnp.where(own_q[h] == q, 1 - own_c[h], own_c[h])
        cc = first if piece == 0 else 1 - first
        dev = {"epoch": jnp.where(
            h == 0, 4 * y + mod4(x + 1 + 2 * q), 4 * mod4(y + 1 + 2 * q) + x), "blend": b}
        return rdma(
            part.at[4 * h + mod4(pos1[h] + 1 + 2 * q), q, cc], rs.at[h, q, cc],
            sent.at[0], r1s.at[h, q, piece], dev,
        )
    pl.semaphore_wait(barrier, 6)
    for h in range(2):
        local_sums(h)
        for direction in range(2):
            msg1(h, 0, direction).start()
    wait_wave = wave(0)
    for i in (2, 3, 4, 5):
        local_sums(i)
        h, direction = (i - 2) // 2, (i - 2) % 2
        msg1(h, 1, direction).start()
    wait_wave()
    wait_wave = wave(1)
    local_sums(6)
    local_sums(7)
    wait_wave()
    wait_wave = wave(2)

    def add_into(dst, *srcs):
        def body(j, _):
            a, m = lax.div(j, 8), lax.rem(j, 8)
            total = dst[a, m]
            for s in srcs:
                total = total + s[a, m]
            dst[a, m] = total
            return 0

        lax.fori_loop(0, 16, body, 0)
    for h in range(2):
        for direction in range(2):
            msg1(h, 0, direction).wait_recv()
            d = 1 if direction == 0 else 3
            add_into(chunk1(h, d, direction), rf.at[h, direction])
            for piece in range(2):
                sum1(h, direction, piece).start()
    wait_wave()
    wait_wave = wave(3)
    wait_wave()
    wait_wave = wave(4)
    for cp in small[1:3]:
        cp.wait()
    wait_bytes(ft, small_sem.at[2])
    wait_bytes(mo, small_sem.at[3])
    row1 = lax.rem(lax.broadcasted_iota(jnp.int32, (8, 1), 0), 4)
    slots = jnp.zeros((8, 1), jnp.int32)
    for j in range(4):
        slots = jnp.where(row1 == j, count[j], slots)
    live_col = slots.astype(F32)

    def twice(v):
        return jnp.concatenate([v, v], axis=0)

    for k in range(8):
        rows = pl.ds(k, 4, stride=8)
        for t in range(8):
            seen = jnp.where(k < slots, twice(ft[t, rows, :].astype(F32)), 0.0)
            mask[k, t] = seen
            mph[k, t] = twice(mo[t, rows, :]) * seen
    for cpair in range(3):
        for half in range(2):
            rows_c = sp_in[2 * cpair + half]
            sp_s[4 * half : 4 * half + 4, 8 * cpair : 8 * cpair + 8] = rows_c

    at2 = (at_y, at_x)

    def msg2(h, kind, direction, piece):
        d = 1 if direction == 0 else 3
        j = mod4(pos2[h] + (2 if kind == 0 else d))
        part_of = 1 - direction if kind == 1 else direction
        dst = (rf2, rp2, rs2)[kind]
        if piece is None:
            src = red.at[h, lax.div(j, 2), lax.rem(j, 2), pl.ds(4 * part_of, 4)]
            dst, piece = dst.at[h, direction], 0
        else:
            src = red.at[h, lax.div(j, 2), lax.rem(j, 2), pl.ds(4 * part_of + 2 * piece, 2)]
            dst = dst.at[h, direction, pl.ds(2 * piece, 2)]
        arrived = rp_sem.at[1] if kind == 1 else r2.at[h, kind // 2, direction, piece]
        return rdma(src, dst, sent.at[1], arrived, at2[h](d))
    def total1(h, q, cc):
        mine = 4 * h + pos1[h]

        def body(m, _):
            red[h, q, cc, m] = part[mine, q, cc, m] + rs[h, q, cc, m] + rp[h, 1 - q, cc, m]
            return 0

        lax.fori_loop(0, 8, body, 0)

    wait_bytes(rp, rp_sem.at[0])
    wait_wave()
    wait_wave = wave(5)
    for h in range(2):
        sum1(h, 1 - own_q[h], 0).wait_recv()
        total1(h, 1 - own_q[h], own_c[h])
        for piece in range(2):
            for direction in range(2):
                msg2(h, 0, direction, piece).start()
    for h in range(2):
        sum1(h, own_q[h], 0).wait_recv()
        total1(h, own_q[h], 1 - own_c[h])
        sum1(h, 1 - own_q[h], 1).wait_recv()
        total1(h, 1 - own_q[h], 1 - own_c[h])
        for direction in range(2):
            msg2(h, 1, direction, None).start()
    wait_wave()
    wait_wave = wave(6)
    for piece in range(2):
        for h in range(2):
            for direction in range(2):
                msg2(h, 0, direction, piece).wait_recv()
                d = 1 if direction == 0 else 3
                j = mod4(pos2[h] + d)
                for m in (2 * piece, 2 * piece + 1):
                    at = (h, lax.div(j, 2), lax.rem(j, 2), 4 * direction + m)
                    red[at] = red[at] + rf2[h, direction, m]
                msg2(h, 2, direction, piece).start()
    wait_wave()
    wait_wave = wave(7)

    core_to = (lax.rem(y, 2), lax.rem(x, 2))

    quantity = (lax.div(y, 2), lax.div(x, 2))
    tile = (x, 4 + y)

    def msg_z(h, zt):
        return rdma(
            zs.at[h, zt], fin.at[8 * quantity[h] + tile[h]], zsem_s.at[h], zsem_r.at[h],
            {"epoch": b, "blend": 2 * zt + core_to[h]},
        )
    wait_bytes(rp2, rp_sem.at[1])
    here = tuple((core_to[h] == c) & (e == b) for h in range(2))
    for h in range(2):
        sum1(h, own_q[h], 1).wait_recv()
        total1(h, own_q[h], own_c[h])
    wait_wave()
    for piece in range(2):
        for h in range(2):
            for direction in range(2):
                msg2(h, 2, direction, piece).wait_recv()
                for k in (2 * piece, 2 * piece + 1):
                    m = 4 * direction + k
                    zs[h, m] = (
                        red[h, own_q[h], own_c[h], m]
                        + rs2[h, direction, k] + rp2[h, 1 - direction, k]
                    )
                    stays = here[h] & (z == m)

                    @pl.when(stays)
                    def _(h=h, m=m):
                        fin[8 * quantity[h] + tile[h]] = zs[h, m]

                    @pl.when(jnp.logical_not(stays))
                    def _(h=h, m=m):
                        msg_z(h, m).start()
    for h in range(2):

        @pl.when(here[h])
        def _(h=h):
            wait_bytes(fin.at[pl.ds(0, 7)], zsem_r.at[h])

        @pl.when(jnp.logical_not(here[h]))
        def _(h=h):
            wait_bytes(fin.at[pl.ds(0, 8)], zsem_r.at[h])
    for t in range(8):
        for cpair in range(3):
            wsum = fin[8 + t, cpair]
            inv = 1.0 / (1.0 + wsum)
            co[cpair, t] = fin[t, cpair] * inv
            cv[cpair, t] = wsum * inv
    def spread_over_pairs(v):
        return v + pltpu.roll(v, 8, 1) + pltpu.roll(v, 16, 1)

    def lanes_from(v, first):
        moved = v if first == 0 else pltpu.roll(v, 128 - first, 1)
        return jnp.where(lane128 < 8, moved, 0.0)

    lane128 = lax.broadcasted_iota(jnp.int32, (8, LANES), 1)
    spectra = jnp.where(lane128 < 24, sp_s[...], 0.0)
    for it in range(ITERS):
        power = spectra * spectra
        power = lanes_from(power, 0) + lanes_from(power, 8) + lanes_from(power, 16)
        power = power + pltpu.roll(power, 4, 0)
        step = 1.0 / (1.0 + live_col * power)
        s_of = [
            [jnp.broadcast_to(spectra[:, 8 * p + k : 8 * p + k + 1], (8, LANES)) for k in range(8)]
            for p in range(3)
        ]
        step_of = [jnp.broadcast_to(step[:, k : k + 1], (8, LANES)) for k in range(8)]

        def residual_of(planes, t):
            out = []
            for p in range(3):
                model = s_of[p][0] * planes[0]
                for k in range(1, 8):
                    model = model + s_of[p][k] * planes[k]
                out.append(cv[p, t] * (co[p, t] - model))
            return out

        for t in range(8):
            planes = [mph[k, t] for k in range(8)]
            res = residual_of(planes, t)
            for k in range(8):
                grad = s_of[0][k] * res[0] + s_of[1][k] * res[1] + s_of[2][k] * res[2]
                grad = grad + pltpu.roll(grad, 4, 0)
                planes[k] = jnp.maximum(0.0, planes[k] + grad * step_of[k]) * mask[k, t]
                mph[k, t] = planes[k]
            res = residual_of(planes, t)
            for p in range(3):
                rsd[p, t] = res[p]
        payload = jnp.zeros((8, LANES), F32)
        for k in range(8):
            sums = [None] * 4
            for t in range(8):
                plane = mph[k, t]
                terms = [plane * rsd[0, t], plane * rsd[1, t], plane * rsd[2, t], plane * plane]
                sums = [b_ if a_ is None else a_ + b_ for a_, b_ in zip(sums, terms)]
            for p in range(4):
                column = jnp.sum(sums[p], axis=1, keepdims=True)
                payload = jnp.where(lane128 == 8 * p + k, column, payload)
        ar[it, e] = payload
        for dy, dx in FAR_FIRST:
            rdma(
                ar.at[it, e], ar.at[it, e], sent.at[2], asem_r.at[it],
                {"epoch": 4 * mod4(y + dy) + mod4(x + dx), "blend": b},
            ).start()
        if it == ITERS - 1:
            for k in range(8):
                for t in range(8):
                    morph_o[t, pl.ds(k, 4, stride=8), :] = mph[k, t][0:4]
        else:
            for cpair in range(3):
                for t in range(8):
                    for half in range(2):
                        coadd_o[2 * cpair + half, :, pl.ds(LANES * t, LANES)] = co[cpair, t][
                            4 * half : 4 * half + 4
                        ]
        wait_bytes(ar.at[it, pl.ds(0, 15)], asem_r.at[it])
        total = ar[it, 0]
        for d in range(1, 16):
            total = total + ar[it, d]
        norm = spread_over_pairs(lanes_from(total, 24))
        spectra = jnp.where(
            lane128 < 24, jnp.maximum(0.0, spectra + total / (1.0 + live_col * norm)), 0.0
        )
    for cpair in range(3):
        for half in range(2):
            spec_o[2 * cpair + half] = spectra[4 * half : 4 * half + 4, 8 * cpair : 8 * cpair + 8]
    wait_bytes(part.at[pl.ds(0, 6)], sent.at[0])
    wait_bytes(part.at[pl.ds(0, 3), 0], sent.at[1])
    wait_bytes(ar.at[:, pl.ds(0, 15)], sent.at[2])
    for h in range(2):

        @pl.when(here[h])
        def _(h=h):
            wait_bytes(zs.at[h, pl.ds(0, 7)], zsem_s.at[h])

        @pl.when(jnp.logical_not(here[h]))
        def _(h=h):
            wait_bytes(zs.at[h, pl.ds(0, 8)], zsem_s.at[h])


def write_out(coadd, spectra, morphology, coadd_o, spectra_o, morphology_o, sem):
    copies = [
        pltpu.make_async_copy(
            morphology.at[t], morphology_o.at[:, pl.ds(LANES * t, LANES)], sem.at[t]
        )
        for t in range(8)
    ]
    copies.append(pltpu.make_async_copy(coadd, coadd_o, sem.at[8]))
    copies.append(pltpu.make_async_copy(spectra, spectra_o, sem.at[9]))
    for cp in copies:
        cp.start()
    for cp in copies:
        cp.wait()


def on_device(
    visit_flux, visit_precision, visit_live, footprint, source_count, spectra_init, morphology_init
):
    tile = (8, LANES)
    hbm = pl.BlockSpec(memory_space=pl.ANY)
    vmem = pl.BlockSpec(memory_space=pltpu.VMEM)
    dma = pltpu.SemaphoreType.DMA
    coadd, spectra, morphology = pl.pallas_call(
        kernel,
        name="coadd_deblend",
        out_shape=(
            jax.ShapeDtypeStruct((6, 4, 1024), F32),
            jax.ShapeDtypeStruct((6, 4, 8), F32),
            jax.ShapeDtypeStruct((8, 32, LANES), F32),
        ),
        in_specs=[hbm] * 7,
        out_specs=(vmem, vmem, vmem),
        scratch_shapes=[
            pltpu.VMEM((8, 2, 4, 6, 64, LANES), jnp.bfloat16),
            pltpu.VMEM((4, 64), jnp.int32),
            pltpu.VMEM((4, 64, LANES), F32),
            pltpu.VMEM((8, 32, LANES), jnp.int32),
            pltpu.VMEM((8, 32, LANES), F32),
            pltpu.VMEM((6, 4, 8), F32),
            pltpu.VMEM(tile, F32),
            pltpu.VMEM((8, 2, 2, 8, 3, *tile), F32),
            pltpu.VMEM((2, 2, 2, 8, 3, *tile), F32),
            pltpu.VMEM((2, 2, 2, 8, 3, *tile), F32),
            pltpu.VMEM((2, 2, 2, 8, 3, *tile), F32),
            pltpu.VMEM((2, 2, 2, 8, 3, *tile), F32),
            pltpu.VMEM((2, 2, 4, 3, *tile), F32),
            pltpu.VMEM((2, 2, 4, 3, *tile), F32),
            pltpu.VMEM((2, 2, 4, 3, *tile), F32),
            pltpu.VMEM((2, 8, 3, *tile), F32),
            pltpu.VMEM((16, 3, *tile), F32),
            pltpu.VMEM((3, 8, *tile), F32),
            pltpu.VMEM((3, 8, *tile), F32),
            pltpu.VMEM((8, 8, *tile), F32),
            pltpu.VMEM((8, 8, *tile), F32),
            pltpu.VMEM((3, 8, *tile), F32),
            pltpu.VMEM((ITERS, 16, *tile), F32),
            pltpu.SMEM((4,), jnp.int32),
            dma((4,)), dma((5,)), pltpu.SemaphoreType.REGULAR((8,)),
            dma((3,)), dma((2, 2)), dma((2,)), dma((2, 2, 2)), dma((2, 2, 2, 2)),
            dma((2,)), dma((2,)), dma((ITERS,)),
        ],
        compiler_params=pltpu.CompilerParams(
            collective_id=0, has_side_effects=True, vmem_limit_bytes=48 * 1024 * 1024
        ),
    )(
        *[
            pltpu.with_memory_space_constraint(a, pltpu.HBM)
            for a in (
                jnp.transpose(visit_flux, (0, 2, 1, 3)),
                jnp.transpose(visit_precision, (0, 2, 1, 3)),
                visit_live,
                footprint.reshape(32, 1024),
                source_count,
                jnp.transpose(spectra_init, (2, 0, 1)),
                morphology_init.reshape(32, 1024),
            )
        ]
    )
    coadd, spectra, morphology = pl.pallas_call(
        write_out,
        name="write_out",
        out_shape=(
            jax.ShapeDtypeStruct((6, 4, 1024), F32),
            jax.ShapeDtypeStruct((6, 4, 8), F32),
            jax.ShapeDtypeStruct((32, 1024), F32),
        ),
        in_specs=[vmem, vmem, vmem],
        out_specs=(hbm, hbm, hbm),
        scratch_shapes=[dma((10,))],
        compiler_params=pltpu.CompilerParams(vmem_limit_bytes=1024 * 1024),
    )(coadd, spectra, morphology)
    return (
        jnp.transpose(coadd, (1, 0, 2)),
        jnp.transpose(spectra, (1, 2, 0)),
        morphology.reshape(4, 8, 1024),
    )


def solution(mesh):
    in_specs = (
        P("epoch", None, None, "blend"),
        P("epoch", None, None, "blend"),
        P("epoch", None),
        P("blend", None, "epoch"),
        P("blend"),
        P("blend", None, None),
        P("blend", None, "epoch"),
    )
    out_specs = (P("blend", None, "epoch"), P("blend", None, None), P("blend", None, "epoch"))
    return jax.shard_map(
        on_device, mesh=mesh, in_specs=in_specs, out_specs=out_specs, check_vma=False
    )
```

```python
import jax
import jax.numpy as jnp
from jax import lax
from jax.experimental import pallas as pl
from jax.experimental.pallas import tpu as pltpu
from jax.sharding import PartitionSpec as P

ITERS = 2
LANES = 128
F32 = jnp.float32
AWAY = ((4, 2, 6, 0), (3, 5, 1, 7))
HOPS = (0, 1, 2, 1)
FAR_FIRST = sorted(
    [(dy, dx) for dy in range(4) for dx in range(4) if dy or dx],
    key=lambda d: -HOPS[d[0]] - HOPS[d[1]],
)


def kernel(
    flux, prec, live, foot, count_in, spec, morph,
    coadd_o, spec_o, morph_o,
    fp, live_i, live_b, ft, mo, sp_in, sp_s,
    part, rf, rp, rs, red, rf2, rp2, rs2, zs, fin, co, cv, mask, mph, rsd, ar,
    count, load_sem, small_sem, waves, sent, r1, rp_sem, r1s, r2, zsem_r, asem_r,
):
    e = lax.axis_index("epoch")
    b = lax.axis_index("blend")
    y, x = lax.div(e, 4), lax.rem(e, 4)
    z, c = lax.div(b, 2), lax.rem(b, 2)

    def mod4(v):
        return lax.rem(v, 4)

    def wait_bytes(ref, sem):
        pltpu.make_async_copy(ref, ref, sem).wait()

    order = [
        mod4(x + 2), 4 + mod4(y + 2),
        mod4(x + 1), mod4(x + 3), 4 + mod4(y + 1), 4 + mod4(y + 3),
        x, 4 + y,
    ]
    small = [
        pltpu.make_async_copy(live, live_i, small_sem.at[0]),
        pltpu.make_async_copy(spec, sp_in, small_sem.at[1]),
        pltpu.make_async_copy(count_in, count, small_sem.at[4]),
    ]
    for t in range(8):
        lanes = pl.ds(LANES * t, LANES)
        small.append(pltpu.make_async_copy(foot.at[:, lanes], ft.at[t], small_sem.at[2]))
        small.append(pltpu.make_async_copy(morph.at[:, lanes], mo.at[t], small_sem.at[3]))
    small[0].start()
    loads = []
    for i, t in enumerate(order):
        lanes = pl.ds(pl.multiple_of(t * LANES, LANES), LANES)
        group = min(i, 2) if i < 6 else 3
        pair = (
            pltpu.make_async_copy(flux.at[:, :, :, lanes], fp.at[i, 0], load_sem.at[group]),
            pltpu.make_async_copy(prec.at[:, :, :, lanes], fp.at[i, 1], load_sem.at[group]),
        )
        if i < 2:
            for cp in pair:
                cp.start()
        loads.append(pair)

    barrier = pltpu.get_barrier_semaphore()

    def at_x(d):
        return {"epoch": 4 * y + mod4(x + d), "blend": b}

    def at_y(d):
        return {"epoch": 4 * mod4(y + d) + x, "blend": b}

    def at_z(d):
        return {"epoch": e, "blend": lax.rem(b + 2 * d, 16)}

    other_core = {"epoch": e, "blend": 2 * z + 1 - c}
    for dev in (at_x(1), at_x(3), at_y(1), at_y(3), at_z(7), other_core):
        pl.semaphore_signal(barrier, inc=1, device_id=dev)

    def wave(i):
        to = (
            (at_x(1), at_x(3)), (at_y(1), at_y(3)), (at_y(1), at_y(3)),
            (at_z(1),), (at_z(1), at_z(7)), (at_z(2), at_z(6)), (at_z(1), at_z(7)),
            (other_core,),
        )[i]
        for dev in to:
            pl.semaphore_signal(waves.at[i], inc=1, device_id=dev)
        return lambda: pl.semaphore_wait(waves.at[i], len(to))

    for pair in loads[2:]:
        for cp in pair:
            cp.start()
    for cp in small[1:]:
        cp.start()
    small[0].wait()
    live_f = live_i[...].astype(F32)
    pick = (
        lax.broadcasted_iota(jnp.int32, (4, 4 * LANES), 0)
        == lax.div(lax.broadcasted_iota(jnp.int32, (4, 4 * LANES), 1), LANES)
    ).astype(F32)
    spread = lax.dot_general(
        live_f, pick, (((0,), (0,)), ((), ())), preferred_element_type=F32
    )
    for v in range(4):
        live_b[v] = spread[:, LANES * v : LANES * v + LANES]

    low = lax.broadcasted_iota(jnp.int32, (8, LANES), 0) < 4

    pos2 = (y, x)
    goal2 = (lax.div(z, 2), 2 * lax.rem(z, 2) + c)

    def look_up(values, i):
        out = values[0]
        for k in range(1, len(values)):
            out = jnp.where(i == k, values[k], out)
        return out

    def slot_of(h, q, d):
        chunk = 2 * q + lax.rem(goal2[h] + 1 + d, 2)
        return look_up((3, 1, 0, 2), mod4(chunk - pos2[h] + 4))

    halves = (0, 1, 0, 0, 1, 1, 0, 1)

    def local_sums(i):
        if i in (0, 1, 2, 6):
            wait_bytes(fp.at[pl.ds(i, {2: 4, 6: 2}.get(i, 1))], load_sem.at[min(i, 3)])
        t = order[i]

        def body(g, _):
            rows = pl.ds(pl.multiple_of(g * 16, 16), 16)
            steps = [lax.rem(2 * g + zz - z + 8, 8) for zz in range(2)]
            slots = [[slot_of(halves[i], q, d) for d in steps] for q in range(2)]
            nths = [look_up([AWAY[k % 2].index(k) for k in range(8)], d) for d in steps]
            for cpair in range(3):
                sums = []
                for cc in range(2):
                    band = 2 * cpair + cc
                    num = wsum = None
                    for v in range(4):
                        w = fp[i, 1, v, band, rows, :].astype(F32) * live_b[v, rows, :]
                        n = w * fp[i, 0, v, band, rows, :].astype(F32)
                        num = n if num is None else num + n
                        wsum = w if wsum is None else wsum + w
                    sums.append((num, wsum))
                for q in range(2):
                    for zz in range(2):
                        even = sums[0][q][8 * zz : 8 * zz + 8]
                        odd = sums[1][q][8 * zz : 8 * zz + 8]
                        s, n, w = slots[q][zz], lax.rem(nths[zz], 2), lax.div(nths[zz], 2)
                        part[t, 0, s, n, w, cpair] = jnp.where(low, even, pltpu.roll(odd, 4, 0))
                        part[t, 1, s, n, w, cpair] = jnp.where(low, pltpu.roll(even, 4, 0), odd)
            return 0

        lax.fori_loop(0, 4, body, 0)

    def rdma(src, dst, ssem, rsem, dev):
        return pltpu.make_async_remote_copy(
            src, dst, ssem, rsem, device_id=dev, device_id_type=pl.DeviceIdType.MESH
        )

    pos1 = (x, y)
    at1 = (at_x, at_y)

    def chunk1(h, d, q):
        return part.at[4 * h + mod4(pos1[h] + d), q]

    def msg1(h, kind, direction):
        d = 1 if direction == 0 else 3
        if kind == 0:
            src, dst = chunk1(h, 2, direction), rf.at[h, direction]
        else:
            src, dst = chunk1(h, d, 1 - direction), rp.at[h, direction]
        arrived = rp_sem.at[0] if kind == 1 else r1.at[h, direction]
        return rdma(src, dst, sent.at[0], arrived, at1[h](d))

    PIECES = ((0, 1), (1, 2), (3, 1))

    def sum1(h, q, piece):
        slots = pl.ds(*PIECES[piece])
        return rdma(
            part.at[4 * h + mod4(pos1[h] + 1 + 2 * q), q, slots], rs.at[h, q, slots],
            sent.at[0], r1s.at[h, q, piece], at1[h](1 + 2 * q),
        )
    pl.semaphore_wait(barrier, 6)
    for h in range(2):
        local_sums(h)
        for direction in range(2):
            msg1(h, 0, direction).start()
    wait_wave = wave(0)
    for i in (2, 3, 4, 5):
        local_sums(i)
        h, direction = (i - 2) // 2, (i - 2) % 2
        msg1(h, 1, direction).start()
    wait_wave()
    wait_wave = wave(1)
    local_sums(6)
    local_sums(7)
    wait_wave()
    wait_wave = wave(2)

    def add_into(dst, src):
        def body(j, _):
            a, n = lax.div(j, 2), lax.rem(j, 2)
            dst[a, n] = dst[a, n] + src[a, n]
            return 0

        lax.fori_loop(0, 8, body, 0)
    for h in range(2):
        for direction in range(2):
            msg1(h, 0, direction).wait_recv()
            d = 1 if direction == 0 else 3
            add_into(chunk1(h, d, direction), rf.at[h, direction])
            for piece in range(2):
                sum1(h, direction, piece).start()
    wait_wave()
    wait_wave = wave(3)
    wait_wave()
    wait_wave = wave(4)
    for cp in small[1:3]:
        cp.wait()
    wait_bytes(ft, small_sem.at[2])
    wait_bytes(mo, small_sem.at[3])
    row1 = lax.rem(lax.broadcasted_iota(jnp.int32, (8, 1), 0), 4)
    slots = jnp.zeros((8, 1), jnp.int32)
    for j in range(4):
        slots = jnp.where(row1 == j, count[j], slots)
    live_col = slots.astype(F32)

    def twice(v):
        return jnp.concatenate([v, v], axis=0)

    for k in range(8):
        rows = pl.ds(k, 4, stride=8)
        for t in range(8):
            seen = jnp.where(k < slots, twice(ft[t, rows, :].astype(F32)), 0.0)
            mask[k, t] = seen
            mph[k, t] = twice(mo[t, rows, :]) * seen
    for cpair in range(3):
        for half in range(2):
            rows_c = sp_in[2 * cpair + half]
            sp_s[4 * half : 4 * half + 4, 8 * cpair : 8 * cpair + 8] = rows_c

    at2 = (at_y, at_x)

    def msg2(h, kind, direction, piece):
        d = 1 if direction == 0 else 3
        slot = 0 if kind == 0 else 1 + direction
        if kind == 1:
            src, dst = red.at[h, slot, 1 - direction], rp2.at[h, direction]
            arrived = rp_sem.at[1]
        else:
            src = red.at[h, slot, direction, piece]
            dst = (rf2, None, rs2)[kind].at[h, direction, piece]
            arrived = r2.at[h, kind // 2, direction, piece]
        return rdma(src, dst, sent.at[1], arrived, at2[h](d))
    def total1(h, slot):
        mine = 4 * h + pos1[h]

        def body(j, _):
            n, w = lax.div(j, 2), lax.rem(j, 2)
            for q in range(2):
                red[h, slot, n, w, q] = (
                    part[mine, q, slot, n, w] + rs[h, q, slot, n, w] + rp[h, 1 - q, slot, n, w]
                )
            return 0

        lax.fori_loop(0, 4, body, 0)

    wait_bytes(rp, rp_sem.at[0])
    wait_wave()
    wait_wave = wave(5)
    for h in range(2):
        for q in range(2):
            sum1(h, q, 0).wait_recv()
        total1(h, 0)
        for piece in range(2):
            for direction in range(2):
                msg2(h, 0, direction, piece).start()
    for h in range(2):
        for q in range(2):
            sum1(h, q, 2).start()
    wait_wave()
    wait_wave = wave(6)
    for h in range(2):
        for q in range(2):
            sum1(h, q, 1).wait_recv()
        for slot in (1, 2):
            total1(h, slot)
        for direction in range(2):
            msg2(h, 1, direction, None).start()
    for piece in range(2):
        for h in range(2):
            for direction in range(2):
                msg2(h, 0, direction, piece).wait_recv()
                at = (h, 1 + direction, direction, piece)
                red[at] = red[at] + rf2[h, direction, piece]
                msg2(h, 2, direction, piece).start()
    wait_wave()
    wait_wave = wave(7)

    place = (2 * x + lax.div(y, 2), 2 * (4 + y) + lax.div(x, 2))
    odd = [lax.rem(pos2[h] + goal2[h] + 1, 2) for h in range(2)]

    def msg_z(h, n, w, core):
        d = look_up((AWAY[0][2 * w + n], AWAY[1][2 * w + n]), odd[h])
        return rdma(
            zs.at[h, n, w, core], fin.at[place[h]], sent.at[3], zsem_r.at[0],
            {"epoch": b, "blend": 2 * lax.rem(z + d, 8) + core},
        )
    for h in range(2):
        for q in range(2):
            sum1(h, q, 2).wait_recv()
        total1(h, 3)
    wait_wave()
    wait_bytes(rp2, rp_sem.at[1])
    for piece in range(2):
        for h in range(2):
            for n in range(2):
                msg2(h, 2, n, piece).wait_recv()
                for core in range(2):
                    zs[h, n, piece, core] = (
                        red[h, 3, n, piece, core]
                        + rs2[h, n, piece, core] + rp2[h, 1 - n, piece, core]
                    )
                    msg_z(h, n, piece, core).start()
    wait_bytes(fin, zsem_r.at[0])
    for t in range(8):
        for cpair in range(3):
            wsum = fin[2 * t + 1, cpair]
            inv = 1.0 / (1.0 + wsum)
            co[cpair, t] = fin[2 * t, cpair] * inv
            cv[cpair, t] = wsum * inv
    def spread_over_pairs(v):
        return v + pltpu.roll(v, 8, 1) + pltpu.roll(v, 16, 1)

    def lanes_from(v, first):
        moved = v if first == 0 else pltpu.roll(v, 128 - first, 1)
        return jnp.where(lane128 < 8, moved, 0.0)

    lane128 = lax.broadcasted_iota(jnp.int32, (8, LANES), 1)
    spectra = jnp.where(lane128 < 24, sp_s[...], 0.0)
    for it in range(ITERS):
        power = spectra * spectra
        power = lanes_from(power, 0) + lanes_from(power, 8) + lanes_from(power, 16)
        power = power + pltpu.roll(power, 4, 0)
        step = 1.0 / (1.0 + live_col * power)
        s_of = [
            [jnp.broadcast_to(spectra[:, 8 * p + k : 8 * p + k + 1], (8, LANES)) for k in range(8)]
            for p in range(3)
        ]
        step_of = [jnp.broadcast_to(step[:, k : k + 1], (8, LANES)) for k in range(8)]

        def residual_of(planes, t):
            out = []
            for p in range(3):
                model = s_of[p][0] * planes[0]
                for k in range(1, 8):
                    model = model + s_of[p][k] * planes[k]
                out.append(cv[p, t] * (co[p, t] - model))
            return out

        for t in range(8):
            planes = [mph[k, t] for k in range(8)]
            res = residual_of(planes, t)
            for k in range(8):
                grad = s_of[0][k] * res[0] + s_of[1][k] * res[1] + s_of[2][k] * res[2]
                grad = grad + pltpu.roll(grad, 4, 0)
                planes[k] = jnp.maximum(0.0, planes[k] + grad * step_of[k]) * mask[k, t]
                mph[k, t] = planes[k]
            res = residual_of(planes, t)
            for p in range(3):
                rsd[p, t] = res[p]
        payload = jnp.zeros((8, LANES), F32)
        for k in range(8):
            sums = [None] * 4
            for t in range(8):
                plane = mph[k, t]
                terms = [plane * rsd[0, t], plane * rsd[1, t], plane * rsd[2, t], plane * plane]
                sums = [b_ if a_ is None else a_ + b_ for a_, b_ in zip(sums, terms)]
            for p in range(4):
                column = jnp.sum(sums[p], axis=1, keepdims=True)
                payload = jnp.where(lane128 == 8 * p + k, column, payload)
        ar[it, e] = payload
        for dy, dx in FAR_FIRST:
            rdma(
                ar.at[it, e], ar.at[it, e], sent.at[2], asem_r.at[it],
                {"epoch": 4 * mod4(y + dy) + mod4(x + dx), "blend": b},
            ).start()
        if it == ITERS - 1:
            for k in range(8):
                for t in range(8):
                    morph_o[t, pl.ds(k, 4, stride=8), :] = mph[k, t][0:4]
        else:
            for cpair in range(3):
                for t in range(8):
                    for half in range(2):
                        coadd_o[2 * cpair + half, :, pl.ds(LANES * t, LANES)] = co[cpair, t][
                            4 * half : 4 * half + 4
                        ]
        wait_bytes(ar.at[it, pl.ds(0, 15)], asem_r.at[it])
        total = ar[it, 0]
        for d in range(1, 16):
            total = total + ar[it, d]
        norm = spread_over_pairs(lanes_from(total, 24))
        spectra = jnp.where(
            lane128 < 24, jnp.maximum(0.0, spectra + total / (1.0 + live_col * norm)), 0.0
        )
    for cpair in range(3):
        for half in range(2):
            spec_o[2 * cpair + half] = spectra[4 * half : 4 * half + 4, 8 * cpair : 8 * cpair + 8]
    wait_bytes(part.at[pl.ds(0, 6)], sent.at[0])
    wait_bytes(part.at[pl.ds(0, 3), 0], sent.at[1])
    wait_bytes(ar.at[:, pl.ds(0, 15)], sent.at[2])
    wait_bytes(zs, sent.at[3])


def write_out(coadd, spectra, morphology, coadd_o, spectra_o, morphology_o, sem):
    copies = [
        pltpu.make_async_copy(
            morphology.at[t], morphology_o.at[:, pl.ds(LANES * t, LANES)], sem.at[t]
        )
        for t in range(8)
    ]
    copies.append(pltpu.make_async_copy(coadd, coadd_o, sem.at[8]))
    copies.append(pltpu.make_async_copy(spectra, spectra_o, sem.at[9]))
    for cp in copies:
        cp.start()
    for cp in copies:
        cp.wait()


def on_device(
    visit_flux, visit_precision, visit_live, footprint, source_count, spectra_init, morphology_init
):
    tile = (8, LANES)
    hbm = pl.BlockSpec(memory_space=pl.ANY)
    vmem = pl.BlockSpec(memory_space=pltpu.VMEM)
    dma = pltpu.SemaphoreType.DMA
    coadd, spectra, morphology = pl.pallas_call(
        kernel,
        name="coadd_deblend",
        out_shape=(
            jax.ShapeDtypeStruct((6, 4, 1024), F32),
            jax.ShapeDtypeStruct((6, 4, 8), F32),
            jax.ShapeDtypeStruct((8, 32, LANES), F32),
        ),
        in_specs=[hbm] * 7,
        out_specs=(vmem, vmem, vmem),
        scratch_shapes=[
            pltpu.VMEM((8, 2, 4, 6, 64, LANES), jnp.bfloat16),
            pltpu.VMEM((4, 64), jnp.int32),
            pltpu.VMEM((4, 64, LANES), F32),
            pltpu.VMEM((8, 32, LANES), jnp.int32),
            pltpu.VMEM((8, 32, LANES), F32),
            pltpu.VMEM((6, 4, 8), F32),
            pltpu.VMEM(tile, F32),
            pltpu.VMEM((8, 2, 4, 2, 2, 3, *tile), F32),
            pltpu.VMEM((2, 2, 4, 2, 2, 3, *tile), F32),
            pltpu.VMEM((2, 2, 4, 2, 2, 3, *tile), F32),
            pltpu.VMEM((2, 2, 4, 2, 2, 3, *tile), F32),
            pltpu.VMEM((2, 4, 2, 2, 2, 3, *tile), F32),
            pltpu.VMEM((2, 2, 2, 2, 3, *tile), F32),
            pltpu.VMEM((2, 2, 2, 2, 3, *tile), F32),
            pltpu.VMEM((2, 2, 2, 2, 3, *tile), F32),
            pltpu.VMEM((2, 2, 2, 2, 3, *tile), F32),
            pltpu.VMEM((16, 3, *tile), F32),
            pltpu.VMEM((3, 8, *tile), F32),
            pltpu.VMEM((3, 8, *tile), F32),
            pltpu.VMEM((8, 8, *tile), F32),
            pltpu.VMEM((8, 8, *tile), F32),
            pltpu.VMEM((3, 8, *tile), F32),
            pltpu.VMEM((ITERS, 16, *tile), F32),
            pltpu.SMEM((4,), jnp.int32),
            dma((4,)), dma((5,)), pltpu.SemaphoreType.REGULAR((8,)),
            dma((4,)), dma((2, 2)), dma((2,)), dma((2, 2, 3)), dma((2, 2, 2, 2)),
            dma((1,)), dma((ITERS,)),
        ],
        compiler_params=pltpu.CompilerParams(
            collective_id=0, has_side_effects=True, vmem_limit_bytes=48 * 1024 * 1024
        ),
    )(
        *[
            pltpu.with_memory_space_constraint(a, pltpu.HBM)
            for a in (
                jnp.transpose(visit_flux, (0, 2, 1, 3)),
                jnp.transpose(visit_precision, (0, 2, 1, 3)),
                visit_live,
                footprint.reshape(32, 1024),
                source_count,
                jnp.transpose(spectra_init, (2, 0, 1)),
                morphology_init.reshape(32, 1024),
            )
        ]
    )
    coadd, spectra, morphology = pl.pallas_call(
        write_out,
        name="write_out",
        out_shape=(
            jax.ShapeDtypeStruct((6, 4, 1024), F32),
            jax.ShapeDtypeStruct((6, 4, 8), F32),
            jax.ShapeDtypeStruct((32, 1024), F32),
        ),
        in_specs=[vmem, vmem, vmem],
        out_specs=(hbm, hbm, hbm),
        scratch_shapes=[dma((10,))],
        compiler_params=pltpu.CompilerParams(vmem_limit_bytes=1024 * 1024),
    )(coadd, spectra, morphology)
    return (
        jnp.transpose(coadd, (1, 0, 2)),
        jnp.transpose(spectra, (1, 2, 0)),
        morphology.reshape(4, 8, 1024),
    )


def solution(mesh):
    in_specs = (
        P("epoch", None, None, "blend"),
        P("epoch", None, None, "blend"),
        P("epoch", None),
        P("blend", None, "epoch"),
        P("blend"),
        P("blend", None, None),
        P("blend", None, "epoch"),
    )
    out_specs = (P("blend", None, "epoch"), P("blend", None, None), P("blend", None, "epoch"))
    return jax.shard_map(
        on_device, mesh=mesh, in_specs=in_specs, out_specs=out_specs, check_vma=False
    )
```

```python
import jax
import jax.numpy as jnp
from jax import lax
from jax.experimental import pallas as pl
from jax.experimental.pallas import tpu as pltpu
from jax.sharding import PartitionSpec as P

ITERS = 2
LANES = 128
F32 = jnp.float32
AWAY = ((4, 2, 6, 0), (3, 5, 1, 7))
HOPS = (0, 1, 2, 1)
FAR_FIRST = sorted(
    [(dy, dx) for dy in range(4) for dx in range(4) if dy or dx],
    key=lambda d: -HOPS[d[0]] - HOPS[d[1]],
)


def kernel(
    flux, prec, live, foot, count_in, spec, morph,
    coadd_o, spec_o, morph_o,
    fp, live_i, live_b, ft, mo, sp_in, sp_s,
    part, rf, rp, rs, red, rf2, rp2, rs2, zs, fin, co, cv, mask, mph, rsd, ar,
    count, load_sem, small_sem, waves, sent, r1, rp_sem, r1s, r2, zsem_r, asem_r,
):
    e = lax.axis_index("epoch")
    b = lax.axis_index("blend")
    y, x = lax.div(e, 4), lax.rem(e, 4)
    z, c = lax.div(b, 2), lax.rem(b, 2)

    def mod4(v):
        return lax.rem(v, 4)

    def wait_bytes(ref, sem):
        pltpu.make_async_copy(ref, ref, sem).wait()

    order = [
        mod4(x + 2), 4 + mod4(y + 2),
        mod4(x + 1), mod4(x + 3), 4 + mod4(y + 1), 4 + mod4(y + 3),
        x, 4 + y,
    ]
    small = [
        pltpu.make_async_copy(live, live_i, small_sem.at[0]),
        pltpu.make_async_copy(spec, sp_in, small_sem.at[1]),
        pltpu.make_async_copy(count_in, count, small_sem.at[4]),
    ]
    for t in range(8):
        lanes = pl.ds(LANES * t, LANES)
        small.append(pltpu.make_async_copy(foot.at[:, lanes], ft.at[t], small_sem.at[2]))
        small.append(pltpu.make_async_copy(morph.at[:, lanes], mo.at[t], small_sem.at[3]))
    small[0].start()
    loads = []
    for i, t in enumerate(order):
        lanes = pl.ds(pl.multiple_of(t * LANES, LANES), LANES)
        group = min(i, 2) if i < 6 else 3
        pair = (
            pltpu.make_async_copy(flux.at[:, :, :, lanes], fp.at[i, 0], load_sem.at[group]),
            pltpu.make_async_copy(prec.at[:, :, :, lanes], fp.at[i, 1], load_sem.at[group]),
        )
        if i < 2:
            for cp in pair:
                cp.start()
        loads.append(pair)

    barrier = pltpu.get_barrier_semaphore()

    def at_x(d):
        return {"epoch": 4 * y + mod4(x + d), "blend": b}

    def at_y(d):
        return {"epoch": 4 * mod4(y + d) + x, "blend": b}

    def at_z(d):
        return {"epoch": e, "blend": lax.rem(b + 2 * d, 16)}

    other_core = {"epoch": e, "blend": 2 * z + 1 - c}
    for dev in (at_x(1), at_x(3), at_y(1), at_y(3), at_z(7), other_core):
        pl.semaphore_signal(barrier, inc=1, device_id=dev)

    def wave(i):
        to = (
            (at_x(1), at_x(3)), (at_y(1), at_y(3)), (at_y(1), at_y(3)),
            (at_z(1),), (at_z(1), at_z(7)), (at_z(2), at_z(6)), (at_z(1), at_z(7)),
            (other_core,),
        )[i]
        for dev in to:
            pl.semaphore_signal(waves.at[i], inc=1, device_id=dev)
        return lambda: pl.semaphore_wait(waves.at[i], len(to))

    for pair in loads[2:]:
        for cp in pair:
            cp.start()
    for cp in small[1:]:
        cp.start()
    small[0].wait()
    live_f = live_i[...].astype(F32)
    pick = (
        lax.broadcasted_iota(jnp.int32, (4, 4 * LANES), 0)
        == lax.div(lax.broadcasted_iota(jnp.int32, (4, 4 * LANES), 1), LANES)
    ).astype(F32)
    spread = lax.dot_general(
        live_f, pick, (((0,), (0,)), ((), ())), preferred_element_type=F32
    )
    for v in range(4):
        live_b[v] = spread[:, LANES * v : LANES * v + LANES]

    low = lax.broadcasted_iota(jnp.int32, (8, LANES), 0) < 4

    pos2 = (y, x)
    goal2 = (lax.div(z, 2), 2 * lax.rem(z, 2) + c)

    def look_up(values, i):
        out = values[0]
        for k in range(1, len(values)):
            out = jnp.where(i == k, values[k], out)
        return out

    def slot_of(h, q, d):
        chunk = 2 * q + lax.rem(goal2[h] + 1 + d, 2)
        return look_up((3, 1, 0, 2), mod4(chunk - pos2[h] + 4))

    halves = (0, 1, 0, 0, 1, 1, 0, 1)

    def local_sums(i):
        if i in (0, 1, 2, 6):
            wait_bytes(fp.at[pl.ds(i, {2: 4, 6: 2}.get(i, 1))], load_sem.at[min(i, 3)])
        t = order[i]

        def body(g, _):
            rows = pl.ds(pl.multiple_of(g * 16, 16), 16)
            steps = [lax.rem(2 * g + zz - z + 8, 8) for zz in range(2)]
            slots = [[slot_of(halves[i], q, d) for d in steps] for q in range(2)]
            nths = [look_up([AWAY[k % 2].index(k) for k in range(8)], d) for d in steps]
            for cpair in range(3):
                sums = []
                for cc in range(2):
                    band = 2 * cpair + cc
                    num = wsum = None
                    for v in range(4):
                        w = fp[i, 1, v, band, rows, :].astype(F32) * live_b[v, rows, :]
                        n = w * fp[i, 0, v, band, rows, :].astype(F32)
                        num = n if num is None else num + n
                        wsum = w if wsum is None else wsum + w
                    sums.append((num, wsum))
                for q in range(2):
                    for zz in range(2):
                        even = sums[0][q][8 * zz : 8 * zz + 8]
                        odd = sums[1][q][8 * zz : 8 * zz + 8]
                        s, n, w = slots[q][zz], lax.rem(nths[zz], 2), lax.div(nths[zz], 2)
                        part[t, 0, s, n, w, cpair] = jnp.where(low, even, pltpu.roll(odd, 4, 0))
                        part[t, 1, s, n, w, cpair] = jnp.where(low, pltpu.roll(even, 4, 0), odd)
            return 0

        lax.fori_loop(0, 4, body, 0)

    def rdma(src, dst, ssem, rsem, dev):
        return pltpu.make_async_remote_copy(
            src, dst, ssem, rsem, device_id=dev, device_id_type=pl.DeviceIdType.MESH
        )

    pos1 = (x, y)
    at1 = (at_x, at_y)

    def chunk1(h, d, q):
        return part.at[4 * h + mod4(pos1[h] + d), q]

    def msg1(h, kind, direction):
        d = 1 if direction == 0 else 3
        if kind == 0:
            src, dst = chunk1(h, 2, direction), rf.at[h, direction]
        else:
            src, dst = chunk1(h, d, 1 - direction), rp.at[h, direction]
        arrived = rp_sem.at[0] if kind == 1 else r1.at[h, direction]
        return rdma(src, dst, sent.at[0], arrived, at1[h](d))

    PIECES = ((0, 1), (1, 2), (3, 1))

    def sum1(h, q, piece):
        slots = pl.ds(*PIECES[piece])
        return rdma(
            part.at[4 * h + mod4(pos1[h] + 1 + 2 * q), q, slots], rs.at[h, q, slots],
            sent.at[0], r1s.at[h, q, piece], at1[h](1 + 2 * q),
        )
    pl.semaphore_wait(barrier, 6)
    for h in range(2):
        local_sums(h)
        for direction in range(2):
            msg1(h, 0, direction).start()
    wait_wave = wave(0)
    for i in (2, 3, 4, 5):
        local_sums(i)
        h, direction = (i - 2) // 2, (i - 2) % 2
        msg1(h, 1, direction).start()
    wait_wave()
    wait_wave = wave(1)
    local_sums(6)
    local_sums(7)
    wait_wave()
    wait_wave = wave(2)

    def add_into(dst, src):
        def body(j, _):
            a, n = lax.div(j, 2), lax.rem(j, 2)
            dst[a, n] = dst[a, n] + src[a, n]
            return 0

        lax.fori_loop(0, 8, body, 0)
    for h in range(2):
        for direction in range(2):
            msg1(h, 0, direction).wait_recv()
            d = 1 if direction == 0 else 3
            add_into(chunk1(h, d, direction), rf.at[h, direction])
            for piece in range(2):
                sum1(h, direction, piece).start()
    wait_wave()
    wait_wave = wave(3)
    wait_wave()
    wait_wave = wave(4)
    for cp in small[1:3]:
        cp.wait()
    wait_bytes(ft, small_sem.at[2])
    wait_bytes(mo, small_sem.at[3])
    row1 = lax.rem(lax.broadcasted_iota(jnp.int32, (8, 1), 0), 4)
    slots = jnp.zeros((8, 1), jnp.int32)
    for j in range(4):
        slots = jnp.where(row1 == j, count[j], slots)
    live_col = slots.astype(F32)

    def twice(v):
        return jnp.concatenate([v, v], axis=0)

    for k in range(8):
        rows = pl.ds(k, 4, stride=8)
        for t in range(8):
            seen = jnp.where(k < slots, twice(ft[t, rows, :].astype(F32)), 0.0)
            mask[k, t] = seen
            mph[k, t] = twice(mo[t, rows, :]) * seen
    for cpair in range(3):
        for half in range(2):
            rows_c = sp_in[2 * cpair + half]
            sp_s[4 * half : 4 * half + 4, 8 * cpair : 8 * cpair + 8] = rows_c

    at2 = (at_y, at_x)

    def msg2(h, kind, direction, piece):
        d = 1 if direction == 0 else 3
        slot = 0 if kind == 0 else 1 + direction
        if kind == 1:
            src, dst = red.at[h, slot, 1 - direction], rp2.at[h, direction]
            arrived = rp_sem.at[1]
        else:
            src = red.at[h, slot, direction, piece]
            dst = (rf2, None, rs2)[kind].at[h, direction, piece]
            arrived = r2.at[h, kind // 2, direction, piece]
        return rdma(src, dst, sent.at[1], arrived, at2[h](d))
    def total1(h, slot):
        mine = 4 * h + pos1[h]

        def body(j, _):
            n, w = lax.div(j, 2), lax.rem(j, 2)
            for q in range(2):
                red[h, slot, n, w, q] = (
                    part[mine, q, slot, n, w] + rs[h, q, slot, n, w] + rp[h, 1 - q, slot, n, w]
                )
            return 0

        lax.fori_loop(0, 4, body, 0)

    wait_bytes(rp, rp_sem.at[0])
    wait_wave()
    wait_wave = wave(5)
    for h in range(2):
        for q in range(2):
            sum1(h, q, 0).wait_recv()
        total1(h, 0)
        for piece in range(2):
            for direction in range(2):
                msg2(h, 0, direction, piece).start()
    for h in range(2):
        for q in range(2):
            sum1(h, q, 2).start()
    wait_wave()
    wait_wave = wave(6)
    for h in range(2):
        for q in range(2):
            sum1(h, q, 1).wait_recv()
        for slot in (1, 2):
            total1(h, slot)
        for direction in range(2):
            msg2(h, 1, direction, None).start()
    for piece in range(2):
        for h in range(2):
            for direction in range(2):
                msg2(h, 0, direction, piece).wait_recv()
                at = (h, 1 + direction, direction, piece)
                red[at] = red[at] + rf2[h, direction, piece]
                msg2(h, 2, direction, piece).start()
    wait_wave()
    wait_wave = wave(7)

    tile = (x, 4 + y)
    place = (2 * x + lax.div(y, 2), 2 * (4 + y) + lax.div(x, 2))
    odd = [lax.rem(pos2[h] + goal2[h] + 1, 2) for h in range(2)]

    def msg_z(h, n, w, core):
        d = look_up((AWAY[0][2 * w + n], AWAY[1][2 * w + n]), odd[h])
        return rdma(
            zs.at[h, n, w, core], fin.at[place[h]], sent.at[3], zsem_r.at[tile[h]],
            {"epoch": b, "blend": 2 * lax.rem(z + d, 8) + core},
        )
    for h in range(2):
        for q in range(2):
            sum1(h, q, 2).wait_recv()
        total1(h, 3)
    wait_wave()
    wait_bytes(rp2, rp_sem.at[1])
    for piece in range(2):
        for h in range(2):
            for n in range(2):
                msg2(h, 2, n, piece).wait_recv()
                for core in range(2):
                    zs[h, n, piece, core] = (
                        red[h, 3, n, piece, core]
                        + rs2[h, n, piece, core] + rp2[h, 1 - n, piece, core]
                    )
                    msg_z(h, n, piece, core).start()
    arrivals = [first + mod4(at + d) for d in (0, 1, 3, 2) for first, at in ((0, x), (4, y))]

    def take(t):
        wait_bytes(fin.at[pl.ds(2 * t, 2)], zsem_r.at[t])
        for cpair in range(3):
            wsum = fin[2 * t + 1, cpair]
            inv = 1.0 / (1.0 + wsum)
            co[cpair, t] = fin[2 * t, cpair] * inv
            cv[cpair, t] = wsum * inv

    def spread_over_pairs(v):
        return v + pltpu.roll(v, 8, 1) + pltpu.roll(v, 16, 1)

    def lanes_from(v, first):
        moved = v if first == 0 else pltpu.roll(v, 128 - first, 1)
        return jnp.where(lane128 < 8, moved, 0.0)

    lane128 = lax.broadcasted_iota(jnp.int32, (8, LANES), 1)
    row128 = lax.broadcasted_iota(jnp.int32, (8, LANES), 0)
    offset = lane128 - 32 * lax.rem(row128, 4)
    spectra = jnp.where(lane128 < 24, sp_s[...], 0.0)
    for it in range(ITERS):
        power = spectra * spectra
        power = lanes_from(power, 0) + lanes_from(power, 8) + lanes_from(power, 16)
        power = power + pltpu.roll(power, 4, 0)
        step = 1.0 / (1.0 + live_col * power)
        s_of = [
            [jnp.broadcast_to(spectra[:, 8 * p + k : 8 * p + k + 1], (8, LANES)) for k in range(8)]
            for p in range(3)
        ]
        step_of = [jnp.broadcast_to(step[:, k : k + 1], (8, LANES)) for k in range(8)]

        def residual_of(planes, t):
            out = []
            for p in range(3):
                model = s_of[p][0] * planes[0]
                for k in range(1, 8):
                    model = model + s_of[p][k] * planes[k]
                out.append(cv[p, t] * (co[p, t] - model))
            return out

        for t in arrivals if it == 0 else range(8):
            if it == 0:
                take(t)
            planes = [mph[k, t] for k in range(8)]
            res = residual_of(planes, t)
            for k in range(8):
                grad = s_of[0][k] * res[0] + s_of[1][k] * res[1] + s_of[2][k] * res[2]
                grad = grad + pltpu.roll(grad, 4, 0)
                planes[k] = jnp.maximum(0.0, planes[k] + grad * step_of[k]) * mask[k, t]
                mph[k, t] = planes[k]
            res = residual_of(planes, t)
            for p in range(3):
                rsd[p, t] = res[p]
        payload = jnp.zeros((8, LANES), F32)
        for k in range(8):
            sums = [None] * 4
            for t in range(8):
                plane = mph[k, t]
                terms = [plane * rsd[0, t], plane * rsd[1, t], plane * rsd[2, t], plane * plane]
                sums = [b_ if a_ is None else a_ + b_ for a_, b_ in zip(sums, terms)]
            for p in range(4):
                column = jnp.sum(sums[p], axis=1, keepdims=True)
                payload = jnp.where(offset == 8 * p + k, column, payload)
        payload = payload + pltpu.roll(payload, 1, 0)
        payload = payload + pltpu.roll(payload, 2, 0)
        ar[it, e, 0:1] = payload[3:4]
        ar[it, e, 1:2] = payload[7:8]
        for dy, dx in FAR_FIRST:
            rdma(
                ar.at[it, e], ar.at[it, e], sent.at[2], asem_r.at[it],
                {"epoch": 4 * mod4(y + dy) + mod4(x + dx), "blend": b},
            ).start()
        if it == ITERS - 1:
            for k in range(8):
                for t in range(8):
                    morph_o[t, pl.ds(k, 4, stride=8), :] = mph[k, t][0:4]
        else:
            for cpair in range(3):
                for t in range(8):
                    for half in range(2):
                        coadd_o[2 * cpair + half, :, pl.ds(LANES * t, LANES)] = co[cpair, t][
                            4 * half : 4 * half + 4
                        ]
        wait_bytes(ar.at[it, pl.ds(0, 15)], asem_r.at[it])
        packed = ar[it, 0]
        for d in range(1, 16):
            packed = packed + ar[it, d]
        both = jnp.where(
            row128 < 4,
            jnp.broadcast_to(packed[0:1], (8, LANES)),
            jnp.broadcast_to(packed[1:2], (8, LANES)),
        )
        total = both
        for r in range(1, 4):
            total = jnp.where(lax.rem(row128, 4) == r, pltpu.roll(both, LANES - 32 * r, 1), total)
        norm = spread_over_pairs(lanes_from(total, 24))
        spectra = jnp.where(
            lane128 < 24, jnp.maximum(0.0, spectra + total / (1.0 + live_col * norm)), 0.0
        )
    for cpair in range(3):
        for half in range(2):
            spec_o[2 * cpair + half] = spectra[4 * half : 4 * half + 4, 8 * cpair : 8 * cpair + 8]
    wait_bytes(part.at[pl.ds(0, 6)], sent.at[0])
    wait_bytes(part.at[pl.ds(0, 3), 0], sent.at[1])
    wait_bytes(ar.at[:, pl.ds(0, 15)], sent.at[2])
    wait_bytes(zs, sent.at[3])


def write_out(coadd, spectra, morphology, coadd_o, spectra_o, morphology_o, sem):
    copies = [
        pltpu.make_async_copy(
            morphology.at[t], morphology_o.at[:, pl.ds(LANES * t, LANES)], sem.at[t]
        )
        for t in range(8)
    ]
    copies.append(pltpu.make_async_copy(coadd, coadd_o, sem.at[8]))
    copies.append(pltpu.make_async_copy(spectra, spectra_o, sem.at[9]))
    for cp in copies:
        cp.start()
    for cp in copies:
        cp.wait()


def on_device(
    visit_flux, visit_precision, visit_live, footprint, source_count, spectra_init, morphology_init
):
    tile = (8, LANES)
    hbm = pl.BlockSpec(memory_space=pl.ANY)
    vmem = pl.BlockSpec(memory_space=pltpu.VMEM)
    dma = pltpu.SemaphoreType.DMA
    coadd, spectra, morphology = pl.pallas_call(
        kernel,
        name="coadd_deblend",
        out_shape=(
            jax.ShapeDtypeStruct((6, 4, 1024), F32),
            jax.ShapeDtypeStruct((6, 4, 8), F32),
            jax.ShapeDtypeStruct((8, 32, LANES), F32),
        ),
        in_specs=[hbm] * 7,
        out_specs=(vmem, vmem, vmem),
        scratch_shapes=[
            pltpu.VMEM((8, 2, 4, 6, 64, LANES), jnp.bfloat16),
            pltpu.VMEM((4, 64), jnp.int32),
            pltpu.VMEM((4, 64, LANES), F32),
            pltpu.VMEM((8, 32, LANES), jnp.int32),
            pltpu.VMEM((8, 32, LANES), F32),
            pltpu.VMEM((6, 4, 8), F32),
            pltpu.VMEM(tile, F32),
            pltpu.VMEM((8, 2, 4, 2, 2, 3, *tile), F32),
            pltpu.VMEM((2, 2, 4, 2, 2, 3, *tile), F32),
            pltpu.VMEM((2, 2, 4, 2, 2, 3, *tile), F32),
            pltpu.VMEM((2, 2, 4, 2, 2, 3, *tile), F32),
            pltpu.VMEM((2, 4, 2, 2, 2, 3, *tile), F32),
            pltpu.VMEM((2, 2, 2, 2, 3, *tile), F32),
            pltpu.VMEM((2, 2, 2, 2, 3, *tile), F32),
            pltpu.VMEM((2, 2, 2, 2, 3, *tile), F32),
            pltpu.VMEM((2, 2, 2, 2, 3, *tile), F32),
            pltpu.VMEM((16, 3, *tile), F32),
            pltpu.VMEM((3, 8, *tile), F32),
            pltpu.VMEM((3, 8, *tile), F32),
            pltpu.VMEM((8, 8, *tile), F32),
            pltpu.VMEM((8, 8, *tile), F32),
            pltpu.VMEM((3, 8, *tile), F32),
            pltpu.VMEM((ITERS, 16, 2, LANES), F32),
            pltpu.SMEM((4,), jnp.int32),
            dma((4,)), dma((5,)), pltpu.SemaphoreType.REGULAR((8,)),
            dma((4,)), dma((2, 2)), dma((2,)), dma((2, 2, 3)), dma((2, 2, 2, 2)),
            dma((8,)), dma((ITERS,)),
        ],
        compiler_params=pltpu.CompilerParams(
            collective_id=0, has_side_effects=True, vmem_limit_bytes=48 * 1024 * 1024
        ),
    )(
        *[
            pltpu.with_memory_space_constraint(a, pltpu.HBM)
            for a in (
                jnp.transpose(visit_flux, (0, 2, 1, 3)),
                jnp.transpose(visit_precision, (0, 2, 1, 3)),
                visit_live,
                footprint.reshape(32, 1024),
                source_count,
                jnp.transpose(spectra_init, (2, 0, 1)),
                morphology_init.reshape(32, 1024),
            )
        ]
    )
    coadd, spectra, morphology = pl.pallas_call(
        write_out,
        name="write_out",
        out_shape=(
            jax.ShapeDtypeStruct((6, 4, 1024), F32),
            jax.ShapeDtypeStruct((6, 4, 8), F32),
            jax.ShapeDtypeStruct((32, 1024), F32),
        ),
        in_specs=[vmem, vmem, vmem],
        out_specs=(hbm, hbm, hbm),
        scratch_shapes=[dma((10,))],
        compiler_params=pltpu.CompilerParams(vmem_limit_bytes=1024 * 1024),
    )(coadd, spectra, morphology)
    return (
        jnp.transpose(coadd, (1, 0, 2)),
        jnp.transpose(spectra, (1, 2, 0)),
        morphology.reshape(4, 8, 1024),
    )


def solution(mesh):
    in_specs = (
        P("epoch", None, None, "blend"),
        P("epoch", None, None, "blend"),
        P("epoch", None),
        P("blend", None, "epoch"),
        P("blend"),
        P("blend", None, None),
        P("blend", None, "epoch"),
    )
    out_specs = (P("blend", None, "epoch"), P("blend", None, None), P("blend", None, "epoch"))
    return jax.shard_map(
        on_device, mesh=mesh, in_specs=in_specs, out_specs=out_specs, check_vma=False
    )
```
